32 devices in a mesh: seq: 16 (over z, x, core), exp: 2 (over y).
Axes of the slice: x: 2, y: 2, z: 4, core: 2. Of those that a mesh axis runs over, the one named last changes fastest.
Arguments:
- queries: bfloat16 [6144, 1536], P('seq', 'exp'), may hold values from -120 to 120
- key_heads: bfloat16 [6144, 1536], P('seq', 'exp'), may hold values from -6 to 6
- value_heads: bfloat16 [6144, 1024], P('seq', 'exp'), may hold values from -6 to 6
- block_layout: int32 [48, 16], P('seq'), may hold values from 0 to 21, as said below
- out_weight: bfloat16 [1024, 2048], P('exp'), may hold values from -0.1875 to 0.1875
- norm_gain: float32 [2048], replicated, may hold values from 0.5 to 1.5
- expert_ids: int32 [6144, 1], P(('seq', 'exp')), may hold values from 0 to 1; in each aligned block of 192 rows (0 to 191, 192 to 383, ...) at most 144 rows name the same one
- route_weight: float32 [6144, 1], P(('seq', 'exp')), may hold values from 0.1 to 1
- gate_weight: bfloat16 [2, 2048, 704], P('exp'), may hold values from -0.125 to 0.125
- up_weight: bfloat16 [2, 2048, 704], P('exp'), may hold values from -0.125 to 0.125
- down_weight: bfloat16 [2, 704, 2048], P('exp'), may hold values from -0.21875 to 0.21875
Outputs:
- layer_out: bfloat16 [6144, 2048], P(('seq', 'exp'))
The draws below stay inside these ranges and needn't reach their ends.
Inputs may be any that keep to these rules, and one draw needn't show every extreme that they name: `block_layout`: each row holds the offset 0 and 15 other distinct offsets. `expert_ids`: among the 192 tokens of one device in the expert layer (aligned blocks of rows) at most 144 name the same expert.
All inputs are finite; a program needn't handle non-finite values.
Results may differ from the reference program's by a relative error of at most 0.02.
Values may be sent and summed in bfloat16 or wider, within the bound.
No kernel may reach another device: no remote copies, remote signals or barrier semaphores. Data moves between devices by JAX's collectives and lax.ppermute only.
A program may use at most 128 MiB of HBM per device.

```python
import math
import jax
import jax.numpy as jnp
import numpy as np
from jax import lax

D = 2048
QK = 192
VD = 128
FF_E = 704
BLK = 128
TOK_DEV = 192
TOKENS = 6144
HEADS = 8
SPAN = 22
KSEL = 16
CAP = 144
N_EXP = 2


def pair_draw(key):
    base_key = jax.random.fold_in(key, 7)
    query_key, key_key = jax.random.split(base_key, 2)
    query_draw = jnp.clip(jax.random.normal(query_key, (TOKENS, HEADS * QK), jnp.float32), -6.0, 6.0)
    key_draw = jnp.clip(jax.random.normal(key_key, (TOKENS, HEADS * QK), jnp.float32), -6.0, 6.0)
    return (query_draw, key_draw)


def draw_queries(key, part):
    return pair_draw(key)[0].astype(jnp.bfloat16)


def draw_key_heads(key, part):
    return pair_draw(key)[1].astype(jnp.bfloat16)


def draw_block_layout(key, part):
    row_count = TOKENS // BLK
    random_bits = jax.random.randint(jax.random.fold_in(key, 11), (row_count, SPAN - 1), 0, 1 << 20) * SPAN + jnp.arange(SPAN - 1, dtype=jnp.int32)[None, :]
    ordering = jnp.argsort(random_bits, axis=1, stable=True)[:, :KSEL - 1].astype(jnp.int32) + 1
    return jnp.concatenate([jnp.zeros((row_count, 1), jnp.int32), ordering], axis=1)


def shard_levels(stream_key, dims, pieces, smallest, largest):
    def one(axis_at, blocks):
        steps = jax.random.uniform(jax.random.fold_in(jax.random.fold_in(stream_key, 6), axis_at), (blocks,), jnp.float32, smallest / len(pieces), largest / len(pieces))
        return jnp.repeat(jnp.exp(steps), dims[axis_at] // blocks).reshape((-1,) + (1,) * (len(dims) - axis_at - 1))

    loudness = one(*pieces[0])
    for cut in pieces[1:]:
        loudness = loudness * one(*cut)
    return loudness


def routed_block(stream_key, own, number, rows, count, top, reach, lean):
    order = jax.random.permutation(stream_key, count)
    heavy_load, usual = portions_of(count, rows * top, reach, lean, True), portions_of(count, rows * top, reach, lean, False)
    places = jnp.arange(count)

    def named(lengths, turn):
        used = int((lengths > 0).sum())
        fixed = max(1, used // 4)
        moved = fixed + (places - fixed + turn * (used - fixed)) % max(1, count - fixed)
        return jnp.zeros((count,), jnp.int32).at[order[jnp.where(places < fixed, places, moved)]].set(jnp.asarray(lengths, jnp.int32))

    lengths = jnp.where(number % 4 == 0, named(heavy_load, number // 4), named(usual, number - number // 4 - 1))
    mixed = jax.random.permutation(jax.random.fold_in(own, 3), count)
    source_of, receiver = mixed[0:count // 2 * 2:2], mixed[1:count // 2 * 2:2]
    margin = jnp.minimum(lengths[source_of] - 1, reach - lengths[receiver]) // 2
    margin = jnp.where((source_of == order[0]) | (receiver == order[0]) | (lengths[receiver] == 0), 0, jnp.maximum(margin, 0))
    moved = jax.random.randint(jax.random.fold_in(own, 4), (count // 2,), 0, 1 << 20) % (margin + 1)
    lengths = lengths.at[source_of].add(-moved).at[receiver].add(moved)
    items = jnp.searchsorted(jnp.cumsum(lengths), jnp.arange(rows * top), side="right").astype(jnp.int32)
    grid = items.reshape(top, rows).T
    grid = grid[jax.random.permutation(jax.random.fold_in(own, 1), rows)]
    turn = jax.random.randint(jax.random.fold_in(own, 2), (rows, 1), 0, top)
    return jnp.take_along_axis(grid, (jnp.arange(top)[None, :] + turn) % top, axis=1)


def portions_of(number_of, total, bound, skew, full):
    portions = [(1 << 20) // math.isqrt(grade ** skew) + 1 for grade in range(1, number_of + 1)]
    largest = bound if full else min(bound, max(-(-total // number_of), total * portions[0] // sum(portions)))
    least = 1 if total - largest >= number_of - 1 else 0
    counts, surplus = [largest] + [least] * (number_of - 1), total - largest - least * (number_of - 1)
    while surplus > 0:
        movable = [i for i in range(1, number_of) if counts[i] < largest] or [i for i in range(1, number_of) if counts[i] < bound]
        pool, left = sum([portions[i] for i in movable]), surplus
        for i in movable:
            extra = min(bound - counts[i], max(1, left * portions[i] // pool), surplus)
            counts[i] = counts[i] + extra
            surplus = surplus - extra
    return np.array(counts)


def centred(own_key, shape, deviation, most, pieces=(), held_as=jnp.bfloat16):
    entries = deviation * jax.random.normal(own_key, shape, jnp.float32)
    if pieces:
        entries = entries * shard_levels(own_key, shape, pieces, -0.22, 0.18)
    return jnp.clip(entries, -most, most).astype(held_as)


def setup_inputs(seed: int = 0) -> dict:
    keys = jax.random.split(jax.random.key(seed), 12)
    queries = draw_queries(jax.random.fold_in(keys[11], 71), 0)
    key_heads = draw_key_heads(jax.random.fold_in(keys[11], 71), 0)
    value_heads = centred(keys[2], (TOKENS, HEADS * VD), 1.0, 6.0, ((0, 16), (1, 2)))
    block_layout = draw_block_layout(jax.random.fold_in(keys[11], 71), 0)
    out_weight = centred(keys[4], (HEADS * VD, D), (HEADS * VD) ** -0.5, 0.1875, ((0, 2),))
    norm_gain = jnp.clip(1.0 + 0.1 * jax.random.normal(keys[5], (D,), jnp.float32), 0.5, 1.5)
    expert_ids_keys = jax.random.split(jax.random.fold_in(keys[6], 1), TOKENS // TOK_DEV)
    expert_ids_turns = jax.random.permutation(jax.random.fold_in(keys[6], 3), TOKENS // TOK_DEV)
    expert_ids = jax.vmap(lambda own, number: routed_block(jax.random.fold_in(keys[6], 2), own, number, TOK_DEV, N_EXP, 1, CAP, 1))(expert_ids_keys, expert_ids_turns).reshape((TOKENS, 1))
    route_weight = jnp.clip(jnp.exp(math.log(1.0) - 2.3025851 * jax.random.uniform(keys[7], (TOKENS, 1), jnp.float32) ** shard_levels(keys[7], (TOKENS, 1), ((0, 32),), -0.2, 0.2)), 0.1, 1.0)
    gate_weight = centred(keys[8], (N_EXP, D, FF_E), D ** -0.5, 0.125, ((0, 2),))
    up_weight = centred(keys[9], (N_EXP, D, FF_E), D ** -0.5, 0.125, ((0, 2),))
    down_weight = centred(keys[10], (N_EXP, FF_E, D), FF_E ** -0.5, 0.21875, ((0, 2),))
    return {"queries": queries, "key_heads": key_heads, "value_heads": value_heads, "block_layout": block_layout, "out_weight": out_weight, "norm_gain": norm_gain, "expert_ids": expert_ids, "route_weight": route_weight, "gate_weight": gate_weight, "up_weight": up_weight, "down_weight": down_weight}


def attend_block(block_index, queries, key_heads, value_heads, block_layout):
    within = jnp.arange(BLK, dtype=jnp.int32)
    first = block_index * BLK
    query_grid = lax.dynamic_slice_in_dim(queries, first, BLK, 0).astype(jnp.float32).reshape(BLK, HEADS, QK)
    anchor = block_index - block_layout[block_index]
    is_valid = anchor >= 0
    row_index = (jnp.maximum(anchor, 0)[:, None] * BLK + within[None, :]).reshape(-1)
    keys_sel = jnp.take(key_heads, row_index, axis=0).astype(jnp.float32).reshape(KSEL * BLK, HEADS, QK)
    values_sel = jnp.take(value_heads, row_index, axis=0).astype(jnp.float32).reshape(KSEL * BLK, HEADS, VD)
    scores = jnp.einsum('qhd,khd->hqk', query_grid, keys_sel) * QK ** (-0.5)
    key_pos = (anchor[:, None] * BLK + within[None, :]).reshape(-1)
    key_valid = jnp.repeat(is_valid, BLK)
    allowed = key_valid[None, :] & (key_pos[None, :] <= (first + within)[:, None])
    scores = jnp.where(allowed[None], scores, jnp.float32(-1e+30))
    row_peak = lax.optimization_barrier(jnp.max(scores, axis=2, keepdims=True))
    weights = jnp.exp(scores - row_peak)
    attn_probs = (weights / lax.optimization_barrier(jnp.sum(weights, axis=2, keepdims=True))).astype(jnp.bfloat16)
    attn_probs = lax.optimization_barrier(attn_probs).astype(jnp.float32)
    context = jnp.einsum('hqk,khd->qhd', attn_probs, values_sel)
    return context.astype(jnp.bfloat16).reshape(BLK, HEADS * VD)

def expert_apply(arrivals, gate_matrix, up_matrix, down_matrix):
    gate_part = jnp.dot(arrivals, gate_matrix, preferred_element_type=jnp.float32)
    up_part = jnp.dot(arrivals, up_matrix, preferred_element_type=jnp.float32)
    hidden = (jax.nn.silu(gate_part) * up_part).astype(jnp.bfloat16)
    return jnp.dot(hidden, down_matrix, preferred_element_type=jnp.float32).astype(jnp.bfloat16)

def reference(queries, key_heads, value_heads, block_layout, out_weight, norm_gain, expert_ids, route_weight, gate_weight, up_weight, down_weight):
    context = lax.map(lambda block_index: attend_block(block_index, queries, key_heads, value_heads, block_layout), jnp.arange(TOKENS // BLK, dtype=jnp.int32))
    context = context.reshape(TOKENS, HEADS * VD)
    attended = jnp.dot(context, out_weight, preferred_element_type=jnp.float32)
    rescale = lax.rsqrt(lax.optimization_barrier(jnp.mean(attended * attended, axis=1, keepdims=True)) + 1e-06)
    normed = (attended * rescale * norm_gain).astype(jnp.bfloat16)
    route_ids = expert_ids[:, 0]
    combined = jnp.zeros(attended.shape, jnp.float32)
    for expert in range(N_EXP):
        result = expert_apply(normed, gate_weight[expert], up_weight[expert], down_weight[expert]).astype(jnp.float32)
        combined = combined + jnp.where((route_ids == expert)[:, None], result, jnp.float32(0.0))
    return (attended + route_weight * combined).astype(jnp.bfloat16)
```

```python
import functools
import math

import jax
import jax.numpy as jnp
from jax import lax
from jax.experimental import pallas as pl
from jax.experimental.pallas import tpu as pltpu
from jax.sharding import PartitionSpec as P

QK = 192
VD = 128
BLK = 128
SPAN = 22
NEG = -1e30
LOG2E = 1.4426950408889634
F32 = jnp.float32
BF16 = jnp.bfloat16
MIB = 1 << 20


def ceil_to(value, step):
    return -(-value // step) * step


def vmem():
    return pl.BlockSpec(memory_space=pltpu.VMEM)


def smem():
    return pl.BlockSpec(memory_space=pltpu.SMEM)


def params(mib):
    return pltpu.CompilerParams(vmem_limit_bytes=mib * MIB)


def pack_kv_kernel(group, k_ref, v_ref, *refs):
    outs, kt = refs[:group], refs[group]
    own = lax.axis_index("seq") % group
    tokens = k_ref.shape[0]
    for t in range(tokens // BLK):
        rows = slice(t * BLK, (t + 1) * BLK)
        kt[:, rows] = k_ref[rows, :].T
    for d in range(group):
        head = own ^ d
        outs[d][:QK, :] = kt[pl.ds(pl.multiple_of(head * QK, 16), QK), :]
        for t in range(tokens // BLK):
            rows = slice(t * BLK, (t + 1) * BLK)
            outs[d][QK:, rows] = v_ref[rows, pl.ds(pl.multiple_of(head * VD, VD), VD)]


def pack_kv(k, v, group):
    tokens = k.shape[0]
    out = jax.ShapeDtypeStruct((QK + VD, tokens), BF16)
    return pl.pallas_call(
        functools.partial(pack_kv_kernel, group),
        out_shape=[out] * group,
        in_specs=[vmem(), vmem()],
        out_specs=[vmem()] * group,
        scratch_shapes=[pltpu.VMEM((k.shape[1], tokens), BF16)],
        compiler_params=params(8),
        name="pack_kv",
    )(k, v)


def pack_q_kernel(group, phases, layout_ref, q_ref, *refs):
    outs, qt = refs[:group], refs[group]
    seq = lax.axis_index("seq")
    own, plane = seq % group, seq // group
    tokens = q_ref.shape[0]
    blocks, chosen = layout_ref.shape
    plane_blocks = group * blocks
    aug = outs[0].shape[0] - QK
    row = lax.broadcasted_iota(jnp.int32, (aug, BLK), 0)
    phase = jnp.zeros_like(row)
    for p in range(1, phases):
        phase = phase + (row >= p * plane_blocks).astype(jnp.int32)
    exists = (phase <= plane) & (row < phases * plane_blocks)
    for t in range(tokens // BLK):
        rows = slice(t * BLK, (t + 1) * BLK)
        qt[:, rows] = q_ref[rows, :].T
        offset = own * blocks + t + 2 * plane_blocks * phase - row
        hit = offset == layout_ref[t, 0]
        for c in range(1, chosen):
            hit = hit | (offset == layout_ref[t, c])
        mask = jnp.where(hit & exists, F32(0.0), F32(NEG)).astype(BF16)
        for d in range(group):
            outs[d][QK:, rows] = mask
    for d in range(group):
        outs[d][:QK, :] = qt[pl.ds(pl.multiple_of((own ^ d) * QK, 16), QK), :]


def pack_q(q, layout, group, phases):
    tokens = q.shape[0]
    aug = ceil_to(phases * group * layout.shape[0], 16)
    out = jax.ShapeDtypeStruct((QK + aug, tokens), BF16)
    return pl.pallas_call(
        functools.partial(pack_q_kernel, group, phases),
        out_shape=[out] * group,
        in_specs=[smem(), vmem()],
        out_specs=[vmem()] * group,
        scratch_shapes=[pltpu.VMEM((q.shape[1], tokens), BF16)],
        compiler_params=params(8),
        name="pack_q",
    )(layout, q)


def attend_kernel(group, slots, phase, first, last, rows_step, *refs):
    refs = list(refs)

    def take(count):
        taken = refs[:count]
        del refs[:count]
        return taken

    if first:
        q_in = take(group)
    else:
        q_ref, m_in, acc_in = take(3)
    kv = take(len(slots))
    if first:
        q_ref, m_out, acc_out = take(3)
    elif last:
        outs = take(group)
    else:
        m_out, acc_out = take(2)
    kaug, vaug, s_ref = refs
    own = lax.axis_index("seq") % group
    tokens = kv[0].shape[1]
    blocks = tokens // BLK
    aug = kaug.shape[0] - QK
    scale = F32(QK**-0.5 * LOG2E)
    total = group * tokens
    if first:
        depth = q_in[0].shape[0]
        for d in range(group):
            for t in range(blocks):
                rows = slice(d * tokens + t * BLK, d * tokens + (t + 1) * BLK)
                q_ref[rows, :depth] = q_in[d][:, t * BLK : (t + 1) * BLK].T
                if depth < q_ref.shape[1]:
                    q_ref[rows, depth:] = jnp.zeros((BLK, q_ref.shape[1] - depth), BF16)
    row = lax.broadcasted_iota(jnp.int32, (aug, BLK), 0)
    for at, d in enumerate(slots):
        cols = slice(at * tokens, (at + 1) * tokens)
        kaug[:QK, cols] = kv[at][:QK, :]
        for t in range(blocks):
            part = slice(at * tokens + t * BLK, at * tokens + (t + 1) * BLK)
            here = (phase * group + (own ^ d)) * blocks + t
            kaug[QK:, part] = jnp.where(row == here, F32(1.0), F32(0.0)).astype(BF16)
            vaug[part, :VD] = kv[at][QK:, t * BLK : (t + 1) * BLK]
            vaug[part, VD:] = jnp.ones((BLK, VD), BF16)

    def step(i, carry):
        start = pl.multiple_of(i * rows_step, rows_step)
        rows = pl.ds(start, rows_step)
        s_ref[...] = jnp.dot(q_ref[rows, :], kaug[...], preferred_element_type=F32) * scale
        if first:
            lower = lax.broadcasted_iota(jnp.int32, (BLK, BLK), 0) >= lax.broadcasted_iota(
                jnp.int32, (BLK, BLK), 1
            )
            for t in range(rows_step // BLK):
                tile = (slice(t * BLK, (t + 1) * BLK), pl.ds(start + t * BLK, BLK))
                s_ref[tile] = jnp.where(lower, s_ref[tile], F32(NEG))
        s = s_ref[...]
        peak = jnp.max(s, axis=1, keepdims=True)
        if not first:
            before = m_in[rows, :1]
            peak = jnp.maximum(peak, before)
        weights = jnp.exp2(s - peak).astype(BF16)
        acc = jnp.dot(weights, vaug[...], preferred_element_type=F32)
        if not first:
            acc = acc + acc_in[rows, :] * jnp.exp2(before - peak)
        if last:
            result = (acc[:, :VD] / acc[:, VD:]).astype(BF16)
            refs_out[0][rows, :] = result
        else:
            m_out[rows, :] = jnp.broadcast_to(peak, (rows_step, m_out.shape[1]))
            acc_out[rows, :] = acc
        return carry

    if last:
        for d in range(group):
            for t in range(tokens // rows_step):
                i = d * (tokens // rows_step) + t
                rows = slice(i * rows_step, (i + 1) * rows_step)
                s_ref[...] = jnp.dot(q_ref[rows, :], kaug[...], preferred_element_type=F32) * scale
                s = s_ref[...]
                before = m_in[rows, :1]
                peak = jnp.maximum(jnp.max(s, axis=1, keepdims=True), before)
                weights = jnp.exp2(s - peak).astype(BF16)
                acc = jnp.dot(weights, vaug[...], preferred_element_type=F32)
                acc = acc + acc_in[rows, :] * jnp.exp2(before - peak)
                outs[d][t * rows_step : (t + 1) * rows_step, :] = (acc[:, :VD] / acc[:, VD:]).astype(BF16)
    else:
        lax.fori_loop(0, total // rows_step, step, 0)


def attend(group, slots, phase, kv, q_in=None, state=None, last=False):
    first = state is None
    tokens = kv[0].shape[1]
    total = group * tokens
    keys = len(slots) * tokens
    rows_step = 128
    depth = (q_in[0].shape[0] if first else state[0].shape[1])
    depth = ceil_to(depth, 128)
    m_shape = jax.ShapeDtypeStruct((total, 128), F32)
    acc_shape = jax.ShapeDtypeStruct((total, 2 * VD), F32)
    if first:
        inputs = list(q_in)
        outs = [jax.ShapeDtypeStruct((total, depth), BF16), m_shape, acc_shape]
    elif last:
        inputs = list(state)
        outs = [jax.ShapeDtypeStruct((tokens, VD), BF16)] * group
    else:
        inputs = list(state)
        outs = [m_shape, acc_shape]
    inputs = inputs + list(kv)
    return pl.pallas_call(
        functools.partial(attend_kernel, group, slots, phase, first, last, rows_step),
        out_shape=outs,
        in_specs=[vmem()] * len(inputs),
        out_specs=[vmem()] * len(outs),
        scratch_shapes=[
            pltpu.VMEM((depth, keys), BF16),
            pltpu.VMEM((keys, 2 * VD), BF16),
            pltpu.VMEM((rows_step, keys), F32),
        ],
        compiler_params=params(20),
        name=f"attend_{phase}_{slots[0]}",
    )(*inputs)


def hidden_kernel(group, mine, eps, *refs):
    pieces, refs = refs[: 2 * group], refs[2 * group :]
    w_own, w_same, w_swap, gain, gate_w, up_w = refs[:6]
    refs = refs[6:]
    if mine:
        attended_ref, hidden_ref, ctx, att = refs
    else:
        hidden_ref, ctx, att = refs
    seq, part = lax.axis_index("seq"), lax.axis_index("exp")
    own = seq % group
    side = seq % 2
    rows_here = hidden_ref.shape[0]
    which = part if mine else 1 - part
    rows = pl.ds(pl.multiple_of(which * rows_here, 16), rows_here)
    half = group * VD
    for d in range(group):
        at = pl.multiple_of((own ^ d) * VD, VD)
        ctx[:, pl.ds(at, VD)] = pieces[d][rows, :]
        ctx[:, pl.ds(half + at, VD)] = pieces[group + d][rows, :]
    width = w_own.shape[1] // 2
    for at, ref in ((side, w_same), (1 - side, w_swap)):
        cols = pl.ds(pl.multiple_of(at * width, 128), width)
        att[:, cols] = jnp.dot(ctx[:, :half], w_own[:, cols], preferred_element_type=F32) + jnp.dot(
            ctx[:, half:], ref[...], preferred_element_type=F32
        )
    attended = att[...]
    rescale = lax.rsqrt(jnp.mean(attended * attended, axis=1, keepdims=True) + F32(eps))
    normed = (attended * rescale * gain[...]).astype(BF16)
    gate = jnp.dot(normed, gate_w[0], preferred_element_type=F32)
    up = jnp.dot(normed, up_w[0], preferred_element_type=F32)
    hidden_ref[...] = (gate * jax.nn.sigmoid(gate) * up).astype(BF16)
    if mine:
        attended_ref[...] = attended


def hidden_part(group, mine, pieces, w_own, w_same, w_swap, gain, gate_w, up_w):
    tokens = pieces[0].shape[0]
    rows = tokens // 2
    width = w_own.shape[1]
    inputs = list(pieces) + [w_own, w_same, w_swap, gain, gate_w, up_w]
    outs = [jax.ShapeDtypeStruct((rows, gate_w.shape[2]), BF16)]
    if mine:
        outs = [jax.ShapeDtypeStruct((rows, width), F32)] + outs
    return pl.pallas_call(
        functools.partial(hidden_kernel, group, mine, 1e-06),
        out_shape=outs,
        in_specs=[vmem()] * len(inputs),
        out_specs=[vmem()] * len(outs),
        scratch_shapes=[pltpu.VMEM((rows, 2 * group * VD), BF16), pltpu.VMEM((rows, width), F32)],
        compiler_params=params(24),
        name="hidden_own" if mine else "hidden_peer",
    )(*inputs)


def combine_kernel(group, attended, hid_own, hid_peer, ids, weight, down_own, *refs):
    down, out_ref = refs[:group], refs[group]
    own = lax.axis_index("seq") % group
    here = ids[...] == lax.axis_index("exp")
    zero = jnp.zeros(hid_own.shape, F32)
    mine = jnp.where(here, hid_own[...].astype(F32), zero).astype(BF16)
    other = jnp.where(here, zero, hid_peer[...].astype(F32)).astype(BF16)
    width = out_ref.shape[1] // group
    for d in range(group):
        cols = pl.ds(pl.multiple_of((own ^ d) * width, 128), width)
        result = jnp.dot(mine, down_own[0, :, cols], preferred_element_type=F32) + jnp.dot(
            other, down[d][...], preferred_element_type=F32
        )
        result = result.astype(BF16).astype(F32)
        out_ref[:, cols] = (attended[:, cols] + weight[...] * result).astype(BF16)


def combine(group, attended, hid_own, hid_peer, ids, weight, down_own, down):
    inputs = [attended, hid_own, hid_peer, ids, weight, down_own] + list(down)
    return pl.pallas_call(
        functools.partial(combine_kernel, group),
        out_shape=jax.ShapeDtypeStruct(attended.shape, BF16),
        in_specs=[vmem()] * len(inputs),
        out_specs=vmem(),
        compiler_params=params(20),
        name="combine",
    )(*inputs)


def shards(
    queries,
    key_heads,
    value_heads,
    block_layout,
    out_weight,
    norm_gain,
    expert_ids,
    route_weight,
    gate_weight,
    up_weight,
    down_weight,
):
    peers = lax.axis_size("seq")
    seq = lax.axis_index("seq")
    group = value_heads.shape[1] // VD
    blocks = queries.shape[0] // BLK
    plane_blocks = group * blocks
    phases = 1 + -(-(SPAN - 1) // plane_blocks)

    def swap(array, d):
        return lax.ppermute(array, "seq", [(i, i ^ d) for i in range(peers)])

    def across(array):
        return lax.ppermute(array, "exp", [(0, 1), (1, 0)])

    def swap_across(array, d):
        pairs = [(2 * i + e, 2 * (i ^ d) + 1 - e) for i in range(peers) for e in range(2)]
        return lax.ppermute(array, ("seq", "exp"), pairs)

    def forward(array, d, hop):
        reach = plane_blocks * hop - (SPAN - 1)
        pairs = [
            (i, i + group)
            for i in range(peers - group)
            if (((i % group) ^ d) + 1) * blocks - 1 >= reach
        ]
        return lax.ppermute(array, "seq", pairs)

    kv = pack_kv(key_heads, value_heads, group)
    held = [kv[0]] + [swap(kv[d], d) for d in range(1, group)]
    qs = pack_q(queries, block_layout, group, phases)
    qs = [qs[0]] + [swap(qs[d], d) for d in range(1, group)]

    width = out_weight.shape[1] // 2
    side = seq % 2
    w_part = lax.dynamic_slice_in_dim(out_weight, side * width, width, axis=1)
    w_same = across(w_part)
    w_swap = swap(w_same, 1)
    quarter = down_weight.shape[2] // group
    down_part = lax.dynamic_slice_in_dim(down_weight[0], (seq % group) * quarter, quarter, axis=1)
    down0 = across(down_part)
    down2 = swap(down0, 2)
    down1 = swap(down0, 1)
    down3 = swap(down2, 1)

    q_aug, peak, acc = attend(group, tuple(range(group)), 0, held, q_in=qs)
    for hop in range(1, phases):
        held = [forward(held[d], d, hop) for d in range(group)]
        result = attend(
            group, tuple(range(group)), hop, held, state=(q_aug, peak, acc), last=hop == phases - 1
        )
        if hop < phases - 1:
            peak, acc = result
    context = result
    pieces = [context[0]] + [swap(context[d], d) for d in range(1, group)]
    pieces = pieces + [across(context[0])] + [swap_across(context[d], d) for d in range(1, group)]
    gain = norm_gain.reshape(1, -1)
    (hid_out,) = hidden_part(group, False, pieces, out_weight, w_same, w_swap, gain, gate_weight, up_weight)
    hid_peer = across(hid_out)
    attended, hid_own = hidden_part(
        group, True, pieces, out_weight, w_same, w_swap, gain, gate_weight, up_weight
    )
    return combine(
        group, attended, hid_own, hid_peer, expert_ids, route_weight, down_weight, (down0, down1, down2, down3)
    )


def solution(mesh):
    in_specs = (
        P("seq", "exp"),
        P("seq", "exp"),
        P("seq", "exp"),
        P("seq", None),
        P("exp", None),
        P(),
        P(("seq", "exp"), None),
        P(("seq", "exp"), None),
        P("exp", None, None),
        P("exp", None, None),
        P("exp", None, None),
    )
    out_specs = P(("seq", "exp"), None)
    return jax.shard_map(shards, mesh=mesh, in_specs=in_specs, out_specs=out_specs, check_vma=False)
```

```python
import functools

import jax
import jax.numpy as jnp
from jax import lax
from jax.experimental import pallas as pl
from jax.experimental.pallas import tpu as pltpu
from jax.sharding import PartitionSpec as P


QK = 192
VD = 128
BLK = 128
SPAN = 22
NEG = -1e30
LOG2E = 1.4426950408889634
F32 = jnp.float32
BF16 = jnp.bfloat16
MIB = 1 << 20


def ceil_to(value, step):
    return -(-value // step) * step


def vmem():
    return pl.BlockSpec(memory_space=pltpu.VMEM)


def params(mib):
    return pltpu.CompilerParams(vmem_limit_bytes=mib * MIB)


def anywhere():
    return pl.BlockSpec(memory_space=pl.ANY)


def in_hbm(array):
    return pltpu.with_memory_space_constraint(array, pltpu.HBM)


def pack_kv_kernel(group, k_ref, v_ref, *refs):
    outs, (k_buf, kt, sem) = refs[:group], refs[group:]
    own = lax.axis_index("seq") % group
    tokens = k_ref.shape[0]
    blocks = tokens // BLK
    loads = []
    for t in range(blocks):
        rows = slice(t * BLK, (t + 1) * BLK)
        loads.append(pltpu.make_async_copy(k_ref.at[rows, :], k_buf.at[rows, :], sem.at[t]))
    stores = []
    for d in range(group):
        cols = pl.ds(pl.multiple_of((own ^ d) * VD, VD), VD)
        for t in range(blocks):
            rows = slice(t * BLK, (t + 1) * BLK)
            stores.append(
                pltpu.make_async_copy(
                    v_ref.at[rows, cols], outs[d].at[QK : QK + VD, rows], sem.at[blocks * (d + 1) + t]
                )
            )
    for copy in loads + stores:
        copy.start()
    for t in range(blocks):
        rows = slice(t * BLK, (t + 1) * BLK)
        loads[t].wait()
        kt[:, rows] = k_buf[rows, :].T
    for d in range(group):
        outs[d][:QK, :] = kt[pl.ds(pl.multiple_of((own ^ d) * QK, 16), QK), :]
    for copy in stores:
        copy.wait()


def pack_kv(k, v, group):
    tokens = k.shape[0]
    return pl.pallas_call(
        functools.partial(pack_kv_kernel, group),
        out_shape=[pltpu.VMEM((QK + VD, tokens), BF16)] * group,
        in_specs=[anywhere(), anywhere()],
        out_specs=[vmem()] * group,
        scratch_shapes=[
            pltpu.VMEM(k.shape, BF16),
            pltpu.VMEM((k.shape[1], tokens), BF16),
            pltpu.SemaphoreType.DMA(((group + 1) * (tokens // BLK),)),
        ],
        compiler_params=params(8),
        cost_estimate=pl.CostEstimate(flops=1 << 20, transcendentals=0, bytes_accessed=1 << 20),
        name="pack_kv",
    )(in_hbm(k), in_hbm(v))


def pack_q_kernel(group, phases, layout_hbm, q_ref, w_ref, down_ref, after_ref, *refs):
    outs, (w_out, down_out), (layout_ref, q_buf, qt, sem) = refs[:group], refs[group : group + 2], refs[group + 2 :]
    seq = lax.axis_index("seq")
    own, plane = seq % group, seq // group
    tokens = q_ref.shape[0]
    blocks, chosen = layout_ref.shape
    plane_blocks = group * blocks
    aug = outs[0].shape[0] - QK
    width, quarter = w_out.shape[1], down_out.shape[1]
    loads = []
    for t in range(tokens // BLK):
        rows = slice(t * BLK, (t + 1) * BLK)
        loads.append(pltpu.make_async_copy(q_ref.at[rows, :], q_buf.at[rows, :], sem.at[t]))
    layout_load = pltpu.make_async_copy(layout_hbm, layout_ref, sem.at[blocks])
    down_load = pltpu.make_async_copy(
        down_ref.at[0, :, pl.ds(pl.multiple_of(own * quarter, 128), quarter)], down_out, sem.at[blocks + 1]
    )
    w_load = pltpu.make_async_copy(
        w_ref.at[:, pl.ds(pl.multiple_of((seq % 2) * width, 128), width)], w_out, sem.at[blocks + 2]
    )
    for copy in [layout_load] + loads + [down_load, w_load]:
        copy.start()
    row = lax.broadcasted_iota(jnp.int32, (aug, BLK), 0)
    phase = jnp.zeros_like(row)
    for p in range(1, phases):
        phase = phase + (row >= p * plane_blocks).astype(jnp.int32)
    exists = (phase <= plane) & (row < phases * plane_blocks)
    layout_load.wait()
    for t in range(tokens // BLK):
        rows = slice(t * BLK, (t + 1) * BLK)
        offset = own * blocks + t + 2 * plane_blocks * phase - row
        hit = offset == layout_ref[t, 0]
        for c in range(1, chosen):
            hit = hit | (offset == layout_ref[t, c])
        mask = jnp.where(hit & exists, F32(0.0), F32(NEG)).astype(BF16)
        for d in range(group):
            outs[d][QK:, rows] = mask
        loads[t].wait()
        qt[:, rows] = q_buf[rows, :].T
    for d in range(group):
        outs[d][:QK, :] = qt[pl.ds(pl.multiple_of((own ^ d) * QK, 16), QK), :]
    down_load.wait()
    w_load.wait()


def pack_q(q, layout, w, down, earlier, group, phases):
    tokens = q.shape[0]
    aug = ceil_to(phases * group * layout.shape[0], 16)
    w_part = pltpu.VMEM((w.shape[0], w.shape[1] // 2), BF16)
    down_part = pltpu.VMEM((down.shape[1], down.shape[2] // group), BF16)
    return pl.pallas_call(
        functools.partial(pack_q_kernel, group, phases),
        out_shape=[pltpu.VMEM((QK + aug, tokens), BF16)] * group + [w_part, down_part],
        in_specs=[anywhere()] * 5,
        out_specs=[vmem()] * (group + 2),
        scratch_shapes=[
            pltpu.SMEM(layout.shape, jnp.int32),
            pltpu.VMEM(q.shape, BF16),
            pltpu.VMEM((q.shape[1], tokens), BF16),
            pltpu.SemaphoreType.DMA((layout.shape[0] + 3,)),
        ],
        compiler_params=params(8),
        cost_estimate=pl.CostEstimate(flops=1 << 20, transcendentals=0, bytes_accessed=1 << 20),
        name="pack_q",
    )(in_hbm(layout), in_hbm(q), in_hbm(w), in_hbm(down), earlier)


def select_index(values, own):
    picked = jnp.int32(values[0])
    for at in range(1, len(values)):
        picked = jnp.where(own == at, jnp.int32(values[at]), picked)
    return picked


def attend_kernel(group, tables, phase, first, last, shards_seen, rows_step, *refs):
    refs = list(refs)

    def take(count):
        taken = refs[:count]
        del refs[:count]
        return taken

    if first:
        q_in = take(group)
    else:
        q_ref, m_in, acc_in = take(3)
    kv_refs = take(len(tables))
    if first:
        q_ref, m_out, acc_out = take(3)
    elif last:
        outs = take(2 * group)
        context = refs.pop()
    else:
        m_out, acc_out = take(2)
    kaug, vaug, s_ref = refs
    own = lax.axis_index("seq") % group
    tokens = kv_refs[0].shape[1]
    blocks = tokens // BLK
    aug = kaug.shape[0] - QK
    scale = F32(QK**-0.5 * LOG2E)
    if first:
        depth = q_in[0].shape[0]
        for d in range(group):
            for t in range(blocks):
                rows = slice(d * tokens + t * BLK, d * tokens + (t + 1) * BLK)
                q_ref[rows, :depth] = q_in[d][:, t * BLK : (t + 1) * BLK].T
                if depth < q_ref.shape[1]:
                    q_ref[rows, depth:] = jnp.zeros((BLK, q_ref.shape[1] - depth), BF16)
    row = lax.broadcasted_iota(jnp.int32, (aug, BLK), 0)
    at = 0
    for (count, table), ref in zip(tables, kv_refs):
        for c in range(count):
            base = c * (QK + VD)
            kaug[:QK, at * tokens : (at + 1) * tokens] = ref[base : base + QK, :]
            shard = select_index(table[c], own)
            for t in range(blocks):
                part = slice(at * tokens + t * BLK, at * tokens + (t + 1) * BLK)
                here = (phase * group + shard) * blocks + t
                kaug[QK:, part] = jnp.where(row == here, F32(1.0), F32(0.0)).astype(BF16)
                vaug[part, :VD] = ref[base + QK : base + QK + VD, t * BLK : (t + 1) * BLK]
                vaug[part, VD:] = jnp.ones((BLK, VD), BF16)
            at += 1

    def step(rows, slot, diagonal):
        s_now = s_ref.at[slot]
        s_now[...] = jnp.dot(q_ref[rows, :], kaug[...], preferred_element_type=F32)
        if first:
            lower = lax.broadcasted_iota(jnp.int32, (BLK, BLK), 0) >= lax.broadcasted_iota(
                jnp.int32, (BLK, BLK), 1
            )
            for t in range(rows_step // BLK):
                tile = (slice(t * BLK, (t + 1) * BLK), slice(diagonal + t * BLK, diagonal + (t + 1) * BLK))
                s_now[tile] = jnp.where(lower, s_now[tile], F32(NEG))
        peak = jnp.max(s_now[...], axis=1, keepdims=True)
        if not first:
            before = m_in[rows, :1]
            peak = jnp.maximum(peak, before)
        weights = jnp.exp2((s_now[...] - peak) * scale).astype(BF16)
        acc = jnp.dot(weights, vaug[...], preferred_element_type=F32)
        if not first:
            acc = acc + acc_in[rows, :] * jnp.exp2((before - peak) * scale)
        if last:
            context[rows, :] = (acc[:, :VD] / acc[:, VD:]).astype(BF16)
        else:
            m_out[rows, :] = jnp.broadcast_to(peak, (rows_step, m_out.shape[1]))
            acc_out[rows, :] = acc

    per = tokens // rows_step
    count = 0
    for shard in range(group):
        for r in range(per):
            if first:
                start = shard * tokens + r * rows_step
                step(slice(start, start + rows_step), count % 2, start)
                count += 1
                continue
            rows = pl.ds(pl.multiple_of((own ^ shard) * tokens + r * rows_step, rows_step), rows_step)
            if shard in shards_seen:
                step(rows, count % 2, 0)
                count += 1
            elif last:
                context[rows, :] = (acc_in[rows, :VD] / acc_in[rows, VD:]).astype(BF16)
    if last:
        half = tokens // 2
        part = lax.axis_index("exp")
        for d in range(group):
            outs[d][...] = context[d * tokens : (d + 1) * tokens, :]
            at = pl.multiple_of(d * tokens + part * half, 16)
            outs[group + d][...] = context[pl.ds(at, half), :]


def attend(group, tables, phase, kv, q_in=None, state=None, last=False, shards_seen=(), rows_step=128):
    first = state is None
    tokens = kv[0].shape[1]
    total = group * tokens
    keys = sum(count for count, _ in tables) * tokens
    depth = q_in[0].shape[0] if first else state[0].shape[1]
    depth = ceil_to(depth, 128)
    outs = [pltpu.VMEM((total, 128), F32), pltpu.VMEM((total, 2 * VD), F32)]
    scratch = [
        pltpu.VMEM((depth, keys), BF16),
        pltpu.VMEM((keys, 2 * VD), BF16),
        pltpu.VMEM((2, rows_step, keys), F32),
    ]
    aliases = {}
    if first:
        inputs = list(q_in)
        outs = [pltpu.VMEM((total, depth), BF16)] + outs
    elif last:
        inputs = list(state)
        outs = [pltpu.VMEM((tokens, VD), BF16)] * group + [pltpu.VMEM((tokens // 2, VD), BF16)] * group
        scratch = scratch + [pltpu.VMEM((total, VD), BF16)]
    else:
        inputs = list(state)
        aliases = {1: 0, 2: 1}
    inputs = inputs + list(kv)
    queries = total if first else len(shards_seen) * tokens
    return pl.pallas_call(
        functools.partial(attend_kernel, group, tables, phase, first, last, shards_seen, rows_step),
        out_shape=outs,
        in_specs=[vmem()] * len(inputs),
        out_specs=[vmem()] * len(outs),
        scratch_shapes=scratch,
        input_output_aliases=aliases,
        compiler_params=params(20),
        cost_estimate=pl.CostEstimate(
            flops=4 * queries * keys * 256, transcendentals=queries * keys, bytes_accessed=1 << 20
        ),
    )(*inputs)


def gather_kernel(group, plan, *refs):
    parts, outs = refs[: -len(plan)], refs[-len(plan) :]
    own = lax.axis_index("seq") % group
    size = QK + VD
    for g in range(group):

        @pl.when(own == g)
        def _():
            for out, places in zip(outs, plan):
                for at, place in enumerate(places):
                    part, c = place[g]
                    out[at * size : (at + 1) * size, :] = parts[part][c * size : (c + 1) * size, :]


def gather(group, plan, parts):
    outs = [pltpu.VMEM((len(p) * (QK + VD), parts[0].shape[1]), BF16) for p in plan]
    return pl.pallas_call(
        functools.partial(gather_kernel, group, plan),
        out_shape=outs,
        in_specs=[vmem()] * len(parts),
        out_specs=[vmem()] * len(outs),
        compiler_params=params(8),
        cost_estimate=pl.CostEstimate(flops=1 << 20, transcendentals=0, bytes_accessed=1 << 20),
    )(*parts)


def own_tokens_kernel(group, *refs):
    pieces, out_ref = refs[:group], refs[group]
    half = pieces[0].shape[0] // 2
    rows = pl.ds(pl.multiple_of((1 - lax.axis_index("exp")) * half, 16), half)
    for d in range(group):
        out_ref[d * half : (d + 1) * half, :] = pieces[d][rows, :]


def own_tokens(pieces):
    group = len(pieces)
    return pl.pallas_call(
        functools.partial(own_tokens_kernel, group),
        out_shape=pltpu.VMEM((group * pieces[0].shape[0] // 2, pieces[0].shape[1]), BF16),
        in_specs=[vmem()] * group,
        out_specs=vmem(),
        compiler_params=params(8),
        cost_estimate=pl.CostEstimate(flops=1 << 20, transcendentals=0, bytes_accessed=1 << 20),
        name="own_tokens",
    )(*pieces)


def pack_columns(ref, value):
    ref[: value.shape[0], :] = value[:, :128]
    rest = value[:, 128:]
    half = value.shape[0] // 2
    ref[value.shape[0] :, :] = jnp.concatenate([rest[:half], rest[half:]], axis=1)


def unpack_columns(ref, rows):
    rest = ref[rows:, :]
    return jnp.concatenate(
        [ref[:rows, :], jnp.concatenate([rest[:, :64], rest[:, 64:]], axis=0)], axis=1
    )


def hidden_kernel(group, mine, eps, *refs):
    pieces, refs = refs[: group + (1 if mine else group)], refs[group + (1 if mine else group) :]
    w_own, w_same, w_swap, gain, gate_w, up_w = refs[:6]
    refs = refs[6:]
    if mine:
        ids, down_own, attended_ref, partial_ref, ctx, att = refs
    else:
        hidden_ref, ctx, att = refs
    seq, part = lax.axis_index("seq"), lax.axis_index("exp")
    own = seq % group
    side = seq % 2
    rows_here = ctx.shape[0]
    which = part if mine else 1 - part
    rows = pl.ds(pl.multiple_of(which * rows_here, 16), rows_here)
    half = group * VD
    for d in range(group):
        at = pl.multiple_of((own ^ d) * VD, VD)
        ctx[:, pl.ds(at, VD)] = pieces[d][rows, :]
        if mine:
            ctx[:, pl.ds(half + at, VD)] = pieces[group][d * rows_here : (d + 1) * rows_here, :]
        else:
            ctx[:, pl.ds(half + at, VD)] = pieces[group + d][...]
    width = w_own.shape[1] // 2
    for at, ref in ((side, w_same), (1 - side, w_swap)):
        cols = pl.ds(pl.multiple_of(at * width, 128), width)
        att[:, cols] = jnp.dot(ctx[:, :half], w_own[:, cols], preferred_element_type=F32) + jnp.dot(
            ctx[:, half:], ref[...], preferred_element_type=F32
        )
    attended = att[...]
    rescale = lax.rsqrt(jnp.mean(attended * attended, axis=1, keepdims=True) + F32(eps))
    normed = (attended * rescale * gain[...]).astype(BF16)
    across = (((1,), (1,)), ((), ()))
    gate = lax.dot_general(gate_w[0], normed, across, preferred_element_type=F32)
    up = lax.dot_general(up_w[0], normed, across, preferred_element_type=F32)
    hidden = (gate * jax.nn.sigmoid(gate) * up).astype(BF16)
    if mine:
        attended_ref[...] = attended
        routed = jnp.where(ids[...] == part, hidden.astype(F32), jnp.zeros(hidden.shape, F32)).astype(BF16)
        partial_ref[...] = jnp.dot(routed.T, down_own[0], preferred_element_type=F32)
    else:
        pack_columns(hidden_ref, hidden)


def hidden_part(group, pieces, w_own, w_same, w_swap, gain, gate_w, up_w, *extra):
    mine = bool(extra)
    rows = pieces[0].shape[0] // 2
    width = w_own.shape[1]
    inner = gate_w.shape[1]
    inputs = list(pieces) + [w_own, w_same, w_swap, gain, gate_w, up_w] + list(extra)
    if mine:
        outs = [pltpu.VMEM((rows, width), F32)] * 2
    else:
        outs = [pltpu.VMEM((inner * rows // 128, 128), BF16)]
    return pl.pallas_call(
        functools.partial(hidden_kernel, group, mine, 1e-06),
        out_shape=outs,
        in_specs=[vmem()] * len(inputs),
        out_specs=[vmem()] * len(outs),
        scratch_shapes=[pltpu.VMEM((rows, 2 * group * VD), BF16), pltpu.VMEM((rows, width), F32)],
        compiler_params=params(24),
        cost_estimate=pl.CostEstimate(
            flops=2 * rows * width * (2 * group * VD + 2 * inner), transcendentals=rows * inner, bytes_accessed=1 << 20
        ),
        name="hidden_own" if mine else "hidden_peer",
    )(*inputs)


def combine_kernel(group, attended, partial, hid_peer, ids, weight, *refs):
    down, out_ref = refs[:group], refs[group]
    own = lax.axis_index("seq") % group
    here = ids[...] == lax.axis_index("exp")
    hidden = unpack_columns(hid_peer, down[0].shape[0]).astype(F32)
    other = jnp.where(here, jnp.zeros(hidden.shape, F32), hidden).astype(BF16).T
    column = jnp.broadcast_to(weight[...], (128, weight.shape[1])).T[:, :1]
    width = out_ref.shape[1] // group
    for d in range(group):
        cols = pl.ds(pl.multiple_of((own ^ d) * width, 128), width)
        result = partial[:, cols] + jnp.dot(other, down[d][...], preferred_element_type=F32)
        result = result.astype(BF16).astype(F32)
        out_ref[:, cols] = (attended[:, cols] + column * result).astype(BF16)


def combine(group, attended, partial, hid_peer, ids, weight, down):
    inputs = [attended, partial, hid_peer, ids, weight] + list(down)
    return pl.pallas_call(
        functools.partial(combine_kernel, group),
        out_shape=jax.ShapeDtypeStruct(attended.shape, BF16),
        in_specs=[vmem()] * len(inputs),
        out_specs=vmem(),
        compiler_params=params(20),
        cost_estimate=pl.CostEstimate(flops=1 << 20, transcendentals=0, bytes_accessed=1 << 20),
        name="combine",
    )(*inputs)


def after(values, *earlier):
    return lax.optimization_barrier((tuple(values), earlier))[0]


def shards(
    queries,
    key_heads,
    value_heads,
    block_layout,
    out_weight,
    norm_gain,
    expert_ids,
    route_weight,
    gate_weight,
    up_weight,
    down_weight,
):
    peers = lax.axis_size("seq")
    group = value_heads.shape[1] // VD
    blocks = queries.shape[0] // BLK
    plane_blocks = group * blocks
    phases = 1 + -(-(SPAN - 1) // plane_blocks)

    def swap(array, d):
        return lax.ppermute(array, "seq", [(i, i ^ d) for i in range(peers)])

    def across(array):
        return lax.ppermute(array, "exp", [(0, 1), (1, 0)])

    def swap_across(array, d):
        pairs = [(2 * i + e, 2 * (i ^ d) + 1 - e) for i in range(peers) for e in range(2)]
        return lax.ppermute(array, ("seq", "exp"), pairs)

    def forward(array):
        return lax.ppermute(array, "seq", [(i, i + group) for i in range(peers - group)])

    def needed(hop):
        return [
            shard
            for shard in range(group)
            if (shard + 1) * blocks - 1 >= plane_blocks * hop - (SPAN - 1)
        ]

    kv = pack_kv(key_heads, value_heads, group)
    held = [kv[0]] + [swap(kv[d], d) for d in range(1, group)]
    *qs, w_part, down_part = pack_q(
        queries, block_layout, out_weight, down_weight, kv[0], group, phases
    )
    qs = [qs[0]] + [swap(qs[d], d) for d in range(1, group)]
    down0 = across(down_part)
    w_same = across(w_part)

    tables = tuple((1, (tuple(g ^ d for g in range(group)),)) for d in range(group))
    early = group // 2
    joined = gather(group, (tuple(((d, 0),) * group for d in range(early)),), held[:early])[0]
    q_aug, peak, acc = attend(group, tables, 0, held, q_in=qs)
    (down0,) = after((down0,), peak)
    down2 = swap(down0, 2)

    tables = ((early, tuple(tables[d][1][0] for d in range(early))),) + tables[early:]
    parts = [joined] + held[early:]
    for hop in range(1, phases):
        if hop > 1:
            wanted = needed(hop)
            flat = [(at, c, table[c]) for at, (count, table) in enumerate(tables) for c in range(count)]
            chains = []
            for g in range(group):
                there = sorted((f for f in flat if f[2][g] in wanted), key=lambda f: -f[2][g])
                head = [f for f in there if f[0] == 0][:1]
                chains.append(head + [f for f in there if f not in head])
            plans = [
                ((tuple((chains[g][k][0], chains[g][k][1]) for g in range(group)),),) for k in range(len(wanted))
            ]
            tables = tuple(
                (1, (tuple(chains[g][k][2][g] for g in range(group)),)) for k in range(len(wanted))
            )
            parts = [gather(group, plan, parts[:1] if k == 0 else parts)[0] for k, plan in enumerate(plans)]
        parts = [forward(part) for part in parts]

        def seen(those):
            highest = max(max(table[c]) for count, table in those for c in range(count))
            limit = highest * blocks + blocks - 1 + SPAN - 1 - plane_blocks * hop
            return tuple(shard for shard in range(group) if shard * blocks <= limit)

        state = (q_aug, peak, acc)
        if hop < phases - 1:
            peak, acc = attend(group, tables, hop, parts, state=state, shards_seen=seen(tables))
        else:
            peak, acc = attend(
                group, tables[:-1], hop, parts[:-1], state=state, shards_seen=seen(tables[:-1])
            )
            down0, down2 = after((down0, down2), peak)
            down1 = swap(down0, 1)
            down3 = swap(down2, 1)
            context = attend(
                group,
                tables[-1:],
                hop,
                parts[-1:],
                state=(q_aug, peak, acc),
                last=True,
                shards_seen=seen(tables[-1:]),
            )
    (w_same,) = after((w_same,), context[0])
    w_swap = swap(w_same, 1)
    whole, first = context[:group], context[group:]
    same = [whole[0]] + [swap(whole[d], d) for d in range(1, group)]
    other = [across(first[0])] + [swap_across(first[d], d) for d in range(1, group)]
    mine = [across(own_tokens(same))]
    gain = norm_gain.reshape(1, -1)
    weights = (out_weight, w_same, w_swap, gain, gate_weight.swapaxes(1, 2), up_weight.swapaxes(1, 2))
    ids = expert_ids.reshape(1, -1)
    (hid_out,) = hidden_part(group, same + other, *weights)
    hid_peer = across(hid_out)
    attended, partial = hidden_part(group, same + mine, *weights, ids, down_weight)
    return combine(
        group, attended, partial, hid_peer, ids, route_weight.reshape(1, -1), (down0, down1, down2, down3)
    )


def solution(mesh):
    in_specs = (
        P("seq", "exp"),
        P("seq", "exp"),
        P("seq", "exp"),
        P("seq", None),
        P("exp", None),
        P(),
        P(("seq", "exp"), None),
        P(("seq", "exp"), None),
        P("exp", None, None),
        P("exp", None, None),
        P("exp", None, None),
    )
    out_specs = P(("seq", "exp"), None)

    return jax.shard_map(shards, mesh=mesh, in_specs=in_specs, out_specs=out_specs, check_vma=False)
```

```python
import functools

import jax
import jax.numpy as jnp
from jax import lax
from jax.experimental import pallas as pl
from jax.experimental.pallas import tpu as pltpu
from jax.sharding import PartitionSpec as P


QK = 192
VD = 128
BLK = 128
SPAN = 22
NEG = -1e30
LOG2E = 1.4426950408889634
F32 = jnp.float32
BF16 = jnp.bfloat16
MIB = 1 << 20
EXTRA = 16


def ceil_to(value, step):
    return -(-value // step) * step


def vmem():
    return pl.BlockSpec(memory_space=pltpu.VMEM)


def params(mib):
    return pltpu.CompilerParams(vmem_limit_bytes=mib * MIB)


def anywhere():
    return pl.BlockSpec(memory_space=pl.ANY)


def in_hbm(array):
    return pltpu.with_memory_space_constraint(array, pltpu.HBM)


def pack_kv_kernel(group, k_ref, v_ref, *refs):
    outs, (k_buf, kt, sem) = refs[:group], refs[group:]
    own = lax.axis_index("seq") % group
    tokens = k_ref.shape[0]
    blocks = tokens // BLK
    loads = []
    for t in range(blocks):
        rows = slice(t * BLK, (t + 1) * BLK)
        loads.append(pltpu.make_async_copy(k_ref.at[rows, :], k_buf.at[rows, :], sem.at[t]))
    stores = []
    for d in range(group):
        cols = pl.ds(pl.multiple_of((own ^ d) * VD, VD), VD)
        for t in range(blocks):
            rows = slice(t * BLK, (t + 1) * BLK)
            stores.append(
                pltpu.make_async_copy(
                    v_ref.at[rows, cols], outs[d].at[QK : QK + VD, rows], sem.at[blocks * (d + 1) + t]
                )
            )
    for copy in loads + stores:
        copy.start()
    for t in range(blocks):
        rows = slice(t * BLK, (t + 1) * BLK)
        loads[t].wait()
        kt[:, rows] = k_buf[rows, :].T
    for d in range(group):
        outs[d][:QK, :] = kt[pl.ds(pl.multiple_of((own ^ d) * QK, 16), QK), :]
    for copy in stores:
        copy.wait()


def pack_kv(k, v, group):
    tokens = k.shape[0]
    return pl.pallas_call(
        functools.partial(pack_kv_kernel, group),
        out_shape=[pltpu.VMEM((QK + VD, tokens), BF16)] * group,
        in_specs=[anywhere(), anywhere()],
        out_specs=[vmem()] * group,
        scratch_shapes=[
            pltpu.VMEM(k.shape, BF16),
            pltpu.VMEM((k.shape[1], tokens), BF16),
            pltpu.SemaphoreType.DMA(((group + 1) * (tokens // BLK),)),
        ],
        compiler_params=params(8),
        cost_estimate=pl.CostEstimate(flops=1 << 20, transcendentals=0, bytes_accessed=1 << 20),
        name="pack_kv",
    )(in_hbm(k), in_hbm(v))


def pack_q_kernel(group, phases, layout_hbm, q_ref, w_ref, down_ref, after_ref, ids_ref, *refs):
    outs, (w_out, down_out), (layout_ref, q_buf, qt, sem) = refs[:group], refs[group : group + 2], refs[group + 2 :]
    seq = lax.axis_index("seq")
    own, plane = seq % group, seq // group
    tokens = q_ref.shape[0]
    blocks, chosen = layout_ref.shape
    plane_blocks = group * blocks
    aug = outs[0].shape[0] - QK
    width, quarter = w_out.shape[1], down_out.shape[1]
    loads = []
    for t in range(tokens // BLK):
        rows = slice(t * BLK, (t + 1) * BLK)
        loads.append(pltpu.make_async_copy(q_ref.at[rows, :], q_buf.at[rows, :], sem.at[t]))
    layout_load = pltpu.make_async_copy(layout_hbm, layout_ref, sem.at[blocks])
    down_load = pltpu.make_async_copy(
        down_ref.at[0, :, pl.ds(pl.multiple_of(own * quarter, 128), quarter)], down_out, sem.at[blocks + 1]
    )
    w_load = pltpu.make_async_copy(
        w_ref.at[:, pl.ds(pl.multiple_of((seq % 2) * width, 128), width)],
        w_out.at[: w_ref.shape[0], :],
        sem.at[blocks + 2],
    )
    for copy in [layout_load] + loads + [down_load, w_load]:
        copy.start()
    row = lax.broadcasted_iota(jnp.int32, (aug, BLK), 0)
    phase = jnp.zeros_like(row)
    for p in range(1, phases):
        phase = phase + (row >= p * plane_blocks).astype(jnp.int32)
    exists = (phase <= plane) & (row < phases * plane_blocks)
    ids = jnp.broadcast_to(ids_ref[...].astype(F32), (EXTRA, ids_ref.shape[1]))
    w_out[w_ref.shape[0] :, : ids_ref.shape[1]] = ids.astype(BF16)
    layout_load.wait()
    for t in range(tokens // BLK):
        rows = slice(t * BLK, (t + 1) * BLK)
        offset = own * blocks + t + 2 * plane_blocks * phase - row
        hit = offset == layout_ref[t, 0]
        for c in range(1, chosen):
            hit = hit | (offset == layout_ref[t, c])
        mask = jnp.where(hit & exists, F32(0.0), F32(NEG)).astype(BF16)
        for d in range(group):
            outs[d][QK:, rows] = mask
        loads[t].wait()
        qt[:, rows] = q_buf[rows, :].T
    for d in range(group):
        outs[d][:QK, :] = qt[pl.ds(pl.multiple_of((own ^ d) * QK, 16), QK), :]
    down_load.wait()
    w_load.wait()


def pack_q(q, layout, w, down, earlier, ids, group, phases):
    tokens = q.shape[0]
    aug = ceil_to(phases * group * layout.shape[0], 16)
    w_part = pltpu.VMEM((w.shape[0] + EXTRA, w.shape[1] // 2), BF16)
    down_part = pltpu.VMEM((down.shape[1], down.shape[2] // group), BF16)
    return pl.pallas_call(
        functools.partial(pack_q_kernel, group, phases),
        out_shape=[pltpu.VMEM((QK + aug, tokens), BF16)] * group + [w_part, down_part],
        in_specs=[anywhere()] * 5 + [vmem()],
        out_specs=[vmem()] * (group + 2),
        scratch_shapes=[
            pltpu.SMEM(layout.shape, jnp.int32),
            pltpu.VMEM(q.shape, BF16),
            pltpu.VMEM((q.shape[1], tokens), BF16),
            pltpu.SemaphoreType.DMA((layout.shape[0] + 3,)),
        ],
        compiler_params=params(8),
        cost_estimate=pl.CostEstimate(flops=1 << 20, transcendentals=0, bytes_accessed=1 << 20),
        name="pack_q",
    )(in_hbm(layout), in_hbm(q), in_hbm(w), in_hbm(down), earlier, ids)


def select_index(values, own):
    picked = jnp.int32(values[0])
    for at in range(1, len(values)):
        picked = jnp.where(own == at, jnp.int32(values[at]), picked)
    return picked


def attend_kernel(group, tables, phase, first, last, shards_seen, rows_step, *refs):
    refs = list(refs)

    def take(count):
        taken = refs[:count]
        del refs[:count]
        return taken

    if first:
        q_in = take(group)
    else:
        q_ref, m_in, acc_in = take(3)
    kv_refs = take(len(tables))
    if first:
        q_ref, m_out, acc_out = take(3)
    elif last:
        outs = take(2 * group)
        context = refs.pop()
    else:
        m_out, acc_out = take(2)
    kaug, vaug, s_ref = refs
    own = lax.axis_index("seq") % group
    tokens = kv_refs[0].shape[1]
    blocks = tokens // BLK
    aug = kaug.shape[0] - QK
    scale = F32(QK**-0.5 * LOG2E)
    if first:
        depth = q_in[0].shape[0]
        for d in range(group):
            for t in range(blocks):
                rows = slice(d * tokens + t * BLK, d * tokens + (t + 1) * BLK)
                q_ref[rows, :depth] = q_in[d][:, t * BLK : (t + 1) * BLK].T
                if depth < q_ref.shape[1]:
                    q_ref[rows, depth:] = jnp.zeros((BLK, q_ref.shape[1] - depth), BF16)
    row = lax.broadcasted_iota(jnp.int32, (aug, BLK), 0)
    at = 0
    for (count, table), ref in zip(tables, kv_refs):
        for c in range(count):
            base = c * (QK + VD)
            kaug[:QK, at * tokens : (at + 1) * tokens] = ref[base : base + QK, :]
            shard = select_index(table[c], own)
            for t in range(blocks):
                part = slice(at * tokens + t * BLK, at * tokens + (t + 1) * BLK)
                here = (phase * group + shard) * blocks + t
                kaug[QK:, part] = jnp.where(row == here, F32(1.0), F32(0.0)).astype(BF16)
                vaug[part, :VD] = ref[base + QK : base + QK + VD, t * BLK : (t + 1) * BLK]
                vaug[part, VD:] = jnp.ones((BLK, VD), BF16)
            at += 1

    def step(rows, slot, diagonal):
        s_now = s_ref.at[slot]
        s_now[...] = jnp.dot(q_ref[rows, :], kaug[...], preferred_element_type=F32)
        if first:
            lower = lax.broadcasted_iota(jnp.int32, (BLK, BLK), 0) >= lax.broadcasted_iota(
                jnp.int32, (BLK, BLK), 1
            )
            for t in range(rows_step // BLK):
                tile = (slice(t * BLK, (t + 1) * BLK), slice(diagonal + t * BLK, diagonal + (t + 1) * BLK))
                s_now[tile] = jnp.where(lower, s_now[tile], F32(NEG))
        peak = jnp.max(s_now[...], axis=1, keepdims=True)
        if not first:
            before = m_in[rows, :1]
            peak = jnp.maximum(peak, before)
        weights = jnp.exp2((s_now[...] - peak) * scale).astype(BF16)
        acc = jnp.dot(weights, vaug[...], preferred_element_type=F32)
        if not first:
            acc = acc + acc_in[rows, :] * jnp.exp2((before - peak) * scale)
        if last:
            context[rows, :] = (acc[:, :VD] / acc[:, VD:]).astype(BF16)
        else:
            m_out[rows, :] = jnp.broadcast_to(peak, (rows_step, m_out.shape[1]))
            acc_out[rows, :] = acc

    per = tokens // rows_step
    count = 0
    for shard in range(group):
        for r in range(per):
            if first:
                start = shard * tokens + r * rows_step
                step(slice(start, start + rows_step), count % 2, start)
                count += 1
                continue
            rows = pl.ds(pl.multiple_of((own ^ shard) * tokens + r * rows_step, rows_step), rows_step)
            if shard in shards_seen:
                step(rows, count % 2, 0)
                count += 1
            elif last:
                context[rows, :] = (acc_in[rows, :VD] / acc_in[rows, VD:]).astype(BF16)
    if last:
        half = tokens // 2
        part = lax.axis_index("exp")
        for d in range(group):
            outs[d][...] = context[d * tokens : (d + 1) * tokens, :]
            at = pl.multiple_of(d * tokens + part * half, 16)
            outs[group + d][...] = context[pl.ds(at, half), :]


def attend(group, tables, phase, kv, q_in=None, state=None, last=False, shards_seen=(), rows_step=128):
    first = state is None
    tokens = kv[0].shape[1]
    total = group * tokens
    keys = sum(count for count, _ in tables) * tokens
    depth = q_in[0].shape[0] if first else state[0].shape[1]
    depth = ceil_to(depth, 128)
    outs = [pltpu.VMEM((total, 128), F32), pltpu.VMEM((total, 2 * VD), F32)]
    scratch = [
        pltpu.VMEM((depth, keys), BF16),
        pltpu.VMEM((keys, 2 * VD), BF16),
        pltpu.VMEM((2, rows_step, keys), F32),
    ]
    aliases = {}
    if first:
        inputs = list(q_in)
        outs = [pltpu.VMEM((total, depth), BF16)] + outs
    elif last:
        inputs = list(state)
        outs = [pltpu.VMEM((tokens, VD), BF16)] * group + [pltpu.VMEM((tokens // 2, VD), BF16)] * group
        scratch = scratch + [pltpu.VMEM((total, VD), BF16)]
    else:
        inputs = list(state)
        aliases = {1: 0, 2: 1}
    inputs = inputs + list(kv)
    queries = total if first else len(shards_seen) * tokens
    return pl.pallas_call(
        functools.partial(attend_kernel, group, tables, phase, first, last, shards_seen, rows_step),
        out_shape=outs,
        in_specs=[vmem()] * len(inputs),
        out_specs=[vmem()] * len(outs),
        scratch_shapes=scratch,
        input_output_aliases=aliases,
        compiler_params=params(20),
        cost_estimate=pl.CostEstimate(
            flops=4 * queries * keys * 256, transcendentals=queries * keys, bytes_accessed=1 << 20
        ),
    )(*inputs)


def gather_kernel(group, plan, *refs):
    parts, outs = refs[: -len(plan)], refs[-len(plan) :]
    own = lax.axis_index("seq") % group
    size = QK + VD
    for g in range(group):

        @pl.when(own == g)
        def _():
            for out, places in zip(outs, plan):
                for at, place in enumerate(places):
                    part, c = place[g]
                    out[at * size : (at + 1) * size, :] = parts[part][c * size : (c + 1) * size, :]


def gather(group, plan, parts):
    outs = [pltpu.VMEM((len(p) * (QK + VD), parts[0].shape[1]), BF16) for p in plan]
    return pl.pallas_call(
        functools.partial(gather_kernel, group, plan),
        out_shape=outs,
        in_specs=[vmem()] * len(parts),
        out_specs=[vmem()] * len(outs),
        compiler_params=params(8),
        cost_estimate=pl.CostEstimate(flops=1 << 20, transcendentals=0, bytes_accessed=1 << 20),
    )(*parts)


def own_tokens_kernel(group, *refs):
    pieces, out_ref = refs[:group], refs[group]
    half = pieces[0].shape[0] // 2
    rows = pl.ds(pl.multiple_of((1 - lax.axis_index("exp")) * half, 16), half)
    for d in range(group):
        out_ref[d * half : (d + 1) * half, :] = pieces[d][rows, :]


def own_tokens(pieces):
    group = len(pieces)
    return pl.pallas_call(
        functools.partial(own_tokens_kernel, group),
        out_shape=pltpu.VMEM((group * pieces[0].shape[0] // 2, pieces[0].shape[1]), BF16),
        in_specs=[vmem()] * group,
        out_specs=vmem(),
        compiler_params=params(8),
        cost_estimate=pl.CostEstimate(flops=1 << 20, transcendentals=0, bytes_accessed=1 << 20),
        name="own_tokens",
    )(*pieces)


def capacity_of(rows):
    return 3 * rows // 4


def slots_of(member, capacity):
    tokens = member.shape[1]
    before = lax.broadcasted_iota(jnp.int32, (tokens, tokens), 0) <= lax.broadcasted_iota(
        jnp.int32, (tokens, tokens), 1
    )
    counted = jnp.dot(
        jnp.broadcast_to(member, (16, tokens)).astype(BF16), before.astype(F32).astype(BF16), preferred_element_type=F32
    )[:1]
    slot = lax.broadcasted_iota(jnp.int32, (capacity, tokens), 0).astype(F32) + F32(1.0)
    return jnp.where((slot == counted) & (member > F32(0.5)), F32(1.0), F32(0.0))


def pack_columns(ref, value):
    rows, width = value.shape
    full = width // 128
    for c in range(full):
        ref[c * rows : (c + 1) * rows, :] = value[:, c * 128 : (c + 1) * 128].astype(BF16)
    rest = value[:, full * 128 :]
    half = rows // 2
    ref[full * rows :, :] = jnp.concatenate([rest[:half], rest[half:]], axis=1).astype(BF16)


def unpack_columns(ref, rows, width):
    full = width // 128
    rest = ref[full * rows :, :].astype(F32)
    rest = jnp.concatenate([rest[:, :64], rest[:, 64:]], axis=0).astype(BF16)
    return jnp.concatenate([ref[c * rows : (c + 1) * rows, :] for c in range(full)] + [rest], axis=1)


def hidden_kernel(group, mine, eps, *refs):
    pieces, refs = refs[: group + (1 if mine else group)], refs[group + (1 if mine else group) :]
    w_own, w_same, w_swap, gain, gate_w, up_w = refs[:6]
    refs = refs[6:]
    if mine:
        ids, down_own, attended_ref, partial_ref, place_ref, ctx, att = refs
    else:
        hidden_ref, ctx, att = refs
    seq, part = lax.axis_index("seq"), lax.axis_index("exp")
    own = seq % group
    side = seq % 2
    rows_here = ctx.shape[0]
    which = part if mine else 1 - part
    rows = pl.ds(pl.multiple_of(which * rows_here, 16), rows_here)
    half = group * VD
    for d in range(group):
        at = pl.multiple_of((own ^ d) * VD, VD)
        ctx[:, pl.ds(at, VD)] = pieces[d][rows, :]
        if mine:
            ctx[:, pl.ds(half + at, VD)] = pieces[group][d * rows_here : (d + 1) * rows_here, :]
        else:
            ctx[:, pl.ds(half + at, VD)] = pieces[group + d][...]
    width = w_own.shape[1] // 2
    for at, ref in ((side, w_same), (1 - side, w_swap)):
        cols = pl.ds(pl.multiple_of(at * width, 128), width)
        att[:, cols] = jnp.dot(ctx[:, :half], w_own[:, cols], preferred_element_type=F32) + jnp.dot(
            ctx[:, half:], ref[:half, :], preferred_element_type=F32
        )
    attended = att[...]
    rescale = lax.rsqrt(jnp.mean(attended * attended, axis=1, keepdims=True) + F32(eps))
    normed = (attended * rescale * gain[...]).astype(BF16)
    across = (((1,), (1,)), ((), ()))
    gate = lax.dot_general(gate_w[0], normed, across, preferred_element_type=F32)
    up = lax.dot_general(up_w[0], normed, across, preferred_element_type=F32)
    hidden = (gate * jax.nn.sigmoid(gate) * up).astype(BF16)
    if mine:
        attended_ref[...] = attended
        routed = jnp.where(ids[...] == part, hidden.astype(F32), jnp.zeros(hidden.shape, F32)).astype(BF16)
        partial_ref[...] = jnp.dot(routed.T, down_own[0], preferred_element_type=F32)
        away = jnp.where(ids[...] == part, F32(0.0), F32(1.0))
        place_ref[...] = slots_of(away, place_ref.shape[1]).T.astype(BF16)
    else:
        arriving = w_same[half : half + 1, :rows_here].astype(F32)
        member = jnp.where(arriving == part.astype(F32), F32(1.0), F32(0.0))
        place = slots_of(member, capacity_of(rows_here)).astype(BF16)
        chosen = lax.dot_general(place, hidden, across, preferred_element_type=F32)
        pack_columns(hidden_ref, chosen)


def hidden_part(group, pieces, w_own, w_same, w_swap, gain, gate_w, up_w, *extra):
    mine = bool(extra)
    rows = pieces[0].shape[0] // 2
    width = w_own.shape[1]
    inner = gate_w.shape[1]
    inputs = list(pieces) + [w_own, w_same, w_swap, gain, gate_w, up_w] + list(extra)
    if mine:
        outs = [pltpu.VMEM((rows, width), F32)] * 2 + [pltpu.VMEM((rows, capacity_of(rows)), BF16)]
    else:
        outs = [pltpu.VMEM((inner * capacity_of(rows) // 128, 128), BF16)]
    return pl.pallas_call(
        functools.partial(hidden_kernel, group, mine, 1e-06),
        out_shape=outs,
        in_specs=[vmem()] * len(inputs),
        out_specs=[vmem()] * len(outs),
        scratch_shapes=[pltpu.VMEM((rows, 2 * group * VD), BF16), pltpu.VMEM((rows, width), F32)],
        compiler_params=params(24),
        cost_estimate=pl.CostEstimate(
            flops=2 * rows * width * (2 * group * VD + 2 * inner), transcendentals=rows * inner, bytes_accessed=1 << 20
        ),
        name="hidden_own" if mine else "hidden_peer",
    )(*inputs)


def combine_kernel(group, attended, partial, place, hid_peer, weight, *refs):
    down, out_ref, (result_ref, sem) = refs[:group], refs[group], refs[group + 1 :]
    own = lax.axis_index("seq") % group
    hidden = unpack_columns(hid_peer, place.shape[1], down[0].shape[0])
    other = jnp.dot(place[...], hidden, preferred_element_type=F32).astype(BF16)
    column = jnp.broadcast_to(weight[...], (128, weight.shape[1])).T[:, :1]
    width = out_ref.shape[1] // group
    copies = []
    for d in range(group):
        cols = pl.ds(pl.multiple_of((own ^ d) * width, 128), width)
        result = partial[:, cols] + jnp.dot(other, down[d][...], preferred_element_type=F32)
        result = result.astype(BF16).astype(F32)
        here = slice(d * width, (d + 1) * width)
        result_ref[:, here] = (attended[:, cols] + column * result).astype(BF16)
        copies.append(pltpu.make_async_copy(result_ref.at[:, here], out_ref.at[:, cols], sem.at[d]))
        copies[-1].start()
    for copy in copies:
        copy.wait()


def combine(group, attended, partial, place, hid_peer, weight, down):
    inputs = [attended, partial, place, hid_peer, weight] + list(down)
    return pl.pallas_call(
        functools.partial(combine_kernel, group),
        out_shape=jax.ShapeDtypeStruct(attended.shape, BF16),
        in_specs=[vmem()] * len(inputs),
        out_specs=anywhere(),
        scratch_shapes=[pltpu.VMEM(attended.shape, BF16), pltpu.SemaphoreType.DMA((group,))],
        compiler_params=params(20),
        cost_estimate=pl.CostEstimate(flops=1 << 20, transcendentals=0, bytes_accessed=1 << 20),
        name="combine",
    )(*inputs)


def after(values, *earlier):
    return lax.optimization_barrier((tuple(values), earlier))[0]


def shards(
    queries,
    key_heads,
    value_heads,
    block_layout,
    out_weight,
    norm_gain,
    expert_ids,
    route_weight,
    gate_weight,
    up_weight,
    down_weight,
):
    peers = lax.axis_size("seq")
    group = value_heads.shape[1] // VD
    blocks = queries.shape[0] // BLK
    plane_blocks = group * blocks
    phases = 1 + -(-(SPAN - 1) // plane_blocks)

    def swap(array, d):
        return lax.ppermute(array, "seq", [(i, i ^ d) for i in range(peers)])

    def across(array):
        return lax.ppermute(array, "exp", [(0, 1), (1, 0)])

    def swap_across(array, d):
        pairs = [(2 * i + e, 2 * (i ^ d) + 1 - e) for i in range(peers) for e in range(2)]
        return lax.ppermute(array, ("seq", "exp"), pairs)

    def forward(array):
        return lax.ppermute(array, "seq", [(i, i + group) for i in range(peers - group)])

    def needed(hop):
        return [
            shard
            for shard in range(group)
            if (shard + 1) * blocks - 1 >= plane_blocks * hop - (SPAN - 1)
        ]

    ids = expert_ids.reshape(1, -1)
    kv = pack_kv(key_heads, value_heads, group)
    held = [kv[0]] + [swap(kv[d], d) for d in range(1, group)]
    *qs, w_part, down_part = pack_q(
        queries, block_layout, out_weight, down_weight, kv[0], ids, group, phases
    )
    qs = [qs[0]] + [swap(qs[d], d) for d in range(1, group)]
    down0 = across(down_part)
    w_same = across(w_part)

    tables = tuple((1, (tuple(g ^ d for g in range(group)),)) for d in range(group))
    early = group // 2
    joined = gather(group, (tuple(((d, 0),) * group for d in range(early)),), held[:early])[0]
    q_aug, peak, acc = attend(group, tables, 0, held, q_in=qs)
    (down0,) = after((down0,), peak)
    down2 = swap(down0, 2)

    tables = ((early, tuple(tables[d][1][0] for d in range(early))),) + tables[early:]
    parts = [joined] + held[early:]
    for hop in range(1, phases):
        if hop > 1:
            wanted = needed(hop)
            flat = [(at, c, table[c]) for at, (count, table) in enumerate(tables) for c in range(count)]
            chains = []
            for g in range(group):
                there = sorted((f for f in flat if f[2][g] in wanted), key=lambda f: -f[2][g])
                head = [f for f in there if f[0] == 0][:1]
                chains.append(head + [f for f in there if f not in head])
            plans = [
                ((tuple((chains[g][k][0], chains[g][k][1]) for g in range(group)),),) for k in range(len(wanted))
            ]
            tables = tuple(
                (1, (tuple(chains[g][k][2][g] for g in range(group)),)) for k in range(len(wanted))
            )
            parts = [gather(group, plan, parts[:1] if k == 0 else parts)[0] for k, plan in enumerate(plans)]
        parts = [forward(part) for part in parts]

        def seen(those):
            highest = max(max(table[c]) for count, table in those for c in range(count))
            limit = highest * blocks + blocks - 1 + SPAN - 1 - plane_blocks * hop
            return tuple(shard for shard in range(group) if shard * blocks <= limit)

        state = (q_aug, peak, acc)
        if hop < phases - 1:
            peak, acc = attend(group, tables, hop, parts, state=state, shards_seen=seen(tables))
        else:
            peak, acc = attend(
                group, tables[:-1], hop, parts[:-1], state=state, shards_seen=seen(tables[:-1])
            )
            context = attend(
                group,
                tables[-1:],
                hop,
                parts[-1:],
                state=(q_aug, peak, acc),
                last=True,
                shards_seen=seen(tables[-1:]),
            )
    (w_same,) = after((w_same,), context[0])
    w_swap = swap(w_same, 1)
    whole, first = context[:group], context[group:]
    same = [whole[0]] + [swap(whole[d], d) for d in range(1, group)]
    other = [across(first[0])] + [swap_across(first[d], d) for d in range(1, group)]
    mine = [across(own_tokens(same))]
    gain = norm_gain.reshape(1, -1)
    weights = (out_weight, w_same, w_swap, gain, gate_weight.swapaxes(1, 2), up_weight.swapaxes(1, 2))
    (hid_out,) = hidden_part(group, same + other, *weights)
    hid_peer = across(hid_out)
    down0, down2 = after((down0, down2), hid_out)
    down1 = swap(down0, 1)
    down3 = swap(down2, 1)
    attended, partial, place = hidden_part(group, same + mine, *weights, ids, down_weight)
    return combine(
        group, attended, partial, place, hid_peer, route_weight.reshape(1, -1), (down0, down1, down2, down3)
    )


def solution(mesh):
    in_specs = (
        P("seq", "exp"),
        P("seq", "exp"),
        P("seq", "exp"),
        P("seq", None),
        P("exp", None),
        P(),
        P(("seq", "exp"), None),
        P(("seq", "exp"), None),
        P("exp", None, None),
        P("exp", None, None),
        P("exp", None, None),
    )
    out_specs = P(("seq", "exp"), None)

    return jax.shard_map(shards, mesh=mesh, in_specs=in_specs, out_specs=out_specs, check_vma=False)
```

```python
import functools

import jax
import jax.numpy as jnp
from jax import lax
from jax.experimental import pallas as pl
from jax.experimental.pallas import tpu as pltpu
from jax.sharding import PartitionSpec as P


QK = 192
VD = 128
BLK = 128
SPAN = 22
NEG = -1e30
LOG2E = 1.4426950408889634
F32 = jnp.float32
BF16 = jnp.bfloat16
MIB = 1 << 20
EXTRA = 16


def ceil_to(value, step):
    return -(-value // step) * step


def vmem():
    return pl.BlockSpec(memory_space=pltpu.VMEM)


def params(mib):
    return pltpu.CompilerParams(vmem_limit_bytes=mib * MIB)


def anywhere():
    return pl.BlockSpec(memory_space=pl.ANY)


def in_hbm(array):
    return pltpu.with_memory_space_constraint(array, pltpu.HBM)


def pack_kv_kernel(group, k_ref, v_ref, *refs):
    outs, (k_buf, kt, sem) = refs[:group], refs[group:]
    own = lax.axis_index("seq") % group
    tokens = k_ref.shape[0]
    blocks = tokens // BLK
    loads = []
    for t in range(blocks):
        rows = slice(t * BLK, (t + 1) * BLK)
        loads.append(pltpu.make_async_copy(k_ref.at[rows, :], k_buf.at[rows, :], sem.at[t]))
    stores = []
    for d in range(group):
        cols = pl.ds(pl.multiple_of((own ^ d) * VD, VD), VD)
        for t in range(blocks):
            rows = slice(t * BLK, (t + 1) * BLK)
            stores.append(
                pltpu.make_async_copy(
                    v_ref.at[rows, cols], outs[d].at[QK : QK + VD, rows], sem.at[blocks * (d + 1) + t]
                )
            )
    for copy in loads + stores:
        copy.start()
    for t in range(blocks):
        rows = slice(t * BLK, (t + 1) * BLK)
        loads[t].wait()
        kt[:, rows] = k_buf[rows, :].T
    for d in range(group):
        outs[d][:QK, :] = kt[pl.ds(pl.multiple_of((own ^ d) * QK, 16), QK), :]
    for copy in stores:
        copy.wait()


def pack_kv(k, v, group):
    tokens = k.shape[0]
    return pl.pallas_call(
        functools.partial(pack_kv_kernel, group),
        out_shape=[pltpu.VMEM((QK + VD, tokens), BF16)] * group,
        in_specs=[anywhere()] * 2,
        out_specs=[vmem()] * group,
        scratch_shapes=[
            pltpu.VMEM(k.shape, BF16),
            pltpu.VMEM((k.shape[1], tokens), BF16),
            pltpu.SemaphoreType.DMA(((group + 1) * (tokens // BLK),)),
        ],
        compiler_params=params(8),
        cost_estimate=pl.CostEstimate(flops=1 << 20, transcendentals=0, bytes_accessed=1 << 20),
        name="pack_kv",
    )(in_hbm(k), in_hbm(v))


def cut_kernel(group, w_ref, down_ref, ids_ref, after_ref, w_out, down_out, ids_buf, sem):
    seq = lax.axis_index("seq")
    own = seq % group
    width, quarter = w_out.shape[1], down_out.shape[1]
    ids_load = pltpu.make_async_copy(ids_ref, ids_buf, sem.at[0])
    copies = [
        pltpu.make_async_copy(
            down_ref.at[0, :, pl.ds(pl.multiple_of(own * quarter, 128), quarter)], down_out, sem.at[1]
        ),
        pltpu.make_async_copy(
            w_ref.at[:, pl.ds(pl.multiple_of((seq % 2) * width, 128), width)],
            w_out.at[: w_ref.shape[0], :],
            sem.at[2],
        ),
    ]
    for copy in [ids_load] + copies:
        copy.start()
    ids_load.wait()
    ids = jnp.broadcast_to(ids_buf[...].astype(F32), (EXTRA, ids_buf.shape[1]))
    w_out[w_ref.shape[0] :, : ids_buf.shape[1]] = ids.astype(BF16)
    for copy in copies:
        copy.wait()


def cut(w, down, ids, earlier, group):
    return pl.pallas_call(
        functools.partial(cut_kernel, group),
        out_shape=[
            pltpu.VMEM((w.shape[0] + EXTRA, w.shape[1] // 2), BF16),
            pltpu.VMEM((down.shape[1], down.shape[2] // group), BF16),
        ],
        in_specs=[anywhere()] * 4,
        out_specs=[vmem()] * 2,
        scratch_shapes=[pltpu.VMEM(ids.shape, jnp.int32), pltpu.SemaphoreType.DMA((3,))],
        compiler_params=params(8),
        cost_estimate=pl.CostEstimate(flops=1 << 20, transcendentals=0, bytes_accessed=1 << 20),
        name="cut",
    )(in_hbm(w), in_hbm(down), in_hbm(ids), earlier)


def stage_kernel(*refs):
    count = (len(refs) - 2) // 2
    sem = refs[-1]
    copies = [
        pltpu.make_async_copy(refs[at], refs[count + 1 + at], sem.at[at]) for at in range(count)
    ]
    for copy in copies:
        copy.start()
    for copy in copies:
        copy.wait()


def stage(arrays, earlier):
    return pl.pallas_call(
        stage_kernel,
        out_shape=[pltpu.VMEM(a.shape, a.dtype) for a in arrays],
        in_specs=[anywhere()] * (len(arrays) + 1),
        out_specs=[vmem()] * len(arrays),
        scratch_shapes=[pltpu.SemaphoreType.DMA((len(arrays),))],
        compiler_params=params(16),
        cost_estimate=pl.CostEstimate(flops=1 << 20, transcendentals=0, bytes_accessed=1 << 20),
        name="stage",
    )(*[in_hbm(a) for a in arrays], earlier)


def pack_q_kernel(group, phases, layout_hbm, q_ref, after_ref, *refs):
    outs, (layout_ref, q_buf, qt, sem) = refs[:group], refs[group:]
    seq = lax.axis_index("seq")
    own, plane = seq % group, seq // group
    tokens = q_ref.shape[0]
    blocks, chosen = layout_ref.shape
    plane_blocks = group * blocks
    aug = outs[0].shape[0] - QK
    loads = []
    for t in range(tokens // BLK):
        rows = slice(t * BLK, (t + 1) * BLK)
        loads.append(pltpu.make_async_copy(q_ref.at[rows, :], q_buf.at[rows, :], sem.at[t]))
    layout_load = pltpu.make_async_copy(layout_hbm, layout_ref, sem.at[blocks])
    for copy in [layout_load] + loads:
        copy.start()
    row = lax.broadcasted_iota(jnp.int32, (aug, BLK), 0)
    phase = jnp.zeros_like(row)
    for p in range(1, phases):
        phase = phase + (row >= p * plane_blocks).astype(jnp.int32)
    exists = (phase <= plane) & (row < phases * plane_blocks)
    layout_load.wait()
    for t in range(tokens // BLK):
        rows = slice(t * BLK, (t + 1) * BLK)
        offset = own * blocks + t + 2 * plane_blocks * phase - row
        hit = offset == layout_ref[t, 0]
        for c in range(1, chosen):
            hit = hit | (offset == layout_ref[t, c])
        mask = jnp.where(hit & exists, F32(0.0), F32(NEG)).astype(BF16)
        for d in range(group):
            outs[d][QK:, rows] = mask
        loads[t].wait()
        qt[:, rows] = q_buf[rows, :].T
    for d in range(group):
        outs[d][:QK, :] = qt[pl.ds(pl.multiple_of((own ^ d) * QK, 16), QK), :]


def pack_q(q, layout, earlier, group, phases):
    tokens = q.shape[0]
    aug = ceil_to(phases * group * layout.shape[0], 16)
    return pl.pallas_call(
        functools.partial(pack_q_kernel, group, phases),
        out_shape=[pltpu.VMEM((QK + aug, tokens), BF16)] * group,
        in_specs=[anywhere()] * 3,
        out_specs=[vmem()] * group,
        scratch_shapes=[
            pltpu.SMEM(layout.shape, jnp.int32),
            pltpu.VMEM(q.shape, BF16),
            pltpu.VMEM((q.shape[1], tokens), BF16),
            pltpu.SemaphoreType.DMA((layout.shape[0] + 1,)),
        ],
        compiler_params=params(8),
        cost_estimate=pl.CostEstimate(flops=1 << 20, transcendentals=0, bytes_accessed=1 << 20),
        name="pack_q",
    )(in_hbm(layout), in_hbm(q), earlier)


def select_index(values, own):
    picked = jnp.int32(values[0])
    for at in range(1, len(values)):
        picked = jnp.where(own == at, jnp.int32(values[at]), picked)
    return picked


def attend_kernel(group, tables, phase, first, last, shards_seen, finish, rows_step, *refs):
    refs = list(refs)

    def take(count):
        taken = refs[:count]
        del refs[:count]
        return taken

    if first:
        q_in = take(group)
    else:
        q_ref, m_in, acc_in = take(3)
        if last:
            (ready,) = take(1)
    kv_refs = take(len(tables))
    if first:
        q_ref, m_out, acc_out = take(3)
    elif last:
        outs = take(2 * group)
        (context,) = take(1)
    else:
        m_out, acc_out = take(2)
        if finish:
            (context,) = take(1)
    kaug, vaug, s_ref = refs
    own = lax.axis_index("seq") % group
    tokens = kv_refs[0].shape[1]
    blocks = tokens // BLK
    aug = kaug.shape[0] - QK
    scale = F32(QK**-0.5 * LOG2E)
    if first:
        depth = q_in[0].shape[0]
        for d in range(group):
            for t in range(blocks):
                rows = slice(d * tokens + t * BLK, d * tokens + (t + 1) * BLK)
                q_ref[rows, :depth] = q_in[d][:, t * BLK : (t + 1) * BLK].T
                if depth < q_ref.shape[1]:
                    q_ref[rows, depth:] = jnp.zeros((BLK, q_ref.shape[1] - depth), BF16)
    row = lax.broadcasted_iota(jnp.int32, (aug, BLK), 0)
    at = 0
    for (count, table), ref in zip(tables, kv_refs):
        for c in range(count):
            base = c * (QK + VD)
            kaug[:QK, at * tokens : (at + 1) * tokens] = ref[base : base + QK, :]
            shard = select_index(table[c], own)
            for t in range(blocks):
                part = slice(at * tokens + t * BLK, at * tokens + (t + 1) * BLK)
                here = (phase * group + shard) * blocks + t
                kaug[QK:, part] = jnp.where(row == here, F32(1.0), F32(0.0)).astype(BF16)
                vaug[part, :VD] = ref[base + QK : base + QK + VD, t * BLK : (t + 1) * BLK]
                vaug[part, VD:] = jnp.ones((BLK, VD), BF16)
            at += 1

    def step(rows, slot, diagonal, done):
        s_now = s_ref.at[slot]
        s_now[...] = jnp.dot(q_ref[rows, :], kaug[...], preferred_element_type=F32)
        if first:
            lower = lax.broadcasted_iota(jnp.int32, (BLK, BLK), 0) >= lax.broadcasted_iota(
                jnp.int32, (BLK, BLK), 1
            )
            for t in range(rows_step // BLK):
                tile = (slice(t * BLK, (t + 1) * BLK), slice(diagonal + t * BLK, diagonal + (t + 1) * BLK))
                s_now[tile] = jnp.where(lower, s_now[tile], F32(NEG))
        peak = jnp.max(s_now[...], axis=1, keepdims=True)
        if not first:
            before = m_in[rows, :1]
            peak = jnp.maximum(peak, before)
        weights = jnp.exp2((s_now[...] - peak) * scale).astype(BF16)
        acc = jnp.dot(weights, vaug[...], preferred_element_type=F32)
        if not first:
            acc = acc + acc_in[rows, :] * jnp.exp2((before - peak) * scale)
        if done:
            context[rows, :] = (acc[:, :VD] / acc[:, VD:]).astype(BF16)
        else:
            m_out[rows, :] = jnp.broadcast_to(peak, (rows_step, m_out.shape[1]))
            acc_out[rows, :] = acc

    per = tokens // rows_step
    count = 0
    for shard in range(group):
        for r in range(per):
            if first:
                start = shard * tokens + r * rows_step
                step(slice(start, start + rows_step), count % 2, start, False)
                count += 1
                continue
            rows = pl.ds(pl.multiple_of((own ^ shard) * tokens + r * rows_step, rows_step), rows_step)
            if shard in shards_seen:
                step(rows, count % 2, 0, shard in finish)
                count += 1
            elif shard in finish:
                context[rows, :] = (acc_in[rows, :VD] / acc_in[rows, VD:]).astype(BF16)
    if last:
        half = tokens // 2
        part = lax.axis_index("exp")
        for d in range(group):
            outs[d][...] = context[d * tokens : (d + 1) * tokens, :]
            at = pl.multiple_of(d * tokens + part * half, 16)
            outs[group + d][...] = context[pl.ds(at, half), :]


def attend(group, tables, phase, kv, q_in=None, state=None, last=False, shards_seen=(), finish=(), rows_step=128):
    first = state is None
    tokens = kv[0].shape[1]
    total = group * tokens
    keys = sum(count for count, _ in tables) * tokens
    depth = q_in[0].shape[0] if first else state[0].shape[1]
    depth = ceil_to(depth, 128)
    outs = [pltpu.VMEM((total, 128), F32), pltpu.VMEM((total, 2 * VD), F32)]
    scratch = [
        pltpu.VMEM((depth, keys), BF16),
        pltpu.VMEM((keys, 2 * VD), BF16),
        pltpu.VMEM((2, rows_step, keys), F32),
    ]
    aliases = {}
    if first:
        inputs = list(q_in)
        outs = [pltpu.VMEM((total, depth), BF16)] + outs
    elif last:
        inputs = list(state)
        outs = [pltpu.VMEM((tokens, VD), BF16)] * group + [pltpu.VMEM((tokens // 2, VD), BF16)] * group
        outs = outs + [pltpu.VMEM((total, VD), BF16)]
        aliases = {3: 2 * group}
    else:
        inputs = list(state)
        aliases = {1: 0, 2: 1}
        if finish:
            outs = outs + [pltpu.VMEM((total, VD), BF16)]
    inputs = inputs + list(kv)
    queries = total if first else len(shards_seen) * tokens
    return pl.pallas_call(
        functools.partial(attend_kernel, group, tables, phase, first, last, shards_seen, finish, rows_step),
        out_shape=outs,
        in_specs=[vmem()] * len(inputs),
        out_specs=[vmem()] * len(outs),
        scratch_shapes=scratch,
        input_output_aliases=aliases,
        compiler_params=params(20),
        cost_estimate=pl.CostEstimate(
            flops=4 * queries * keys * 256, transcendentals=queries * keys, bytes_accessed=1 << 20
        ),
    )(*inputs)


def gather_kernel(group, plan, *refs):
    parts, outs = refs[: -len(plan)], refs[-len(plan) :]
    own = lax.axis_index("seq") % group
    size = QK + VD
    for g in range(group):

        @pl.when(own == g)
        def _():
            for out, places in zip(outs, plan):
                for at, place in enumerate(places):
                    part, c = place[g]
                    out[at * size : (at + 1) * size, :] = parts[part][c * size : (c + 1) * size, :]


def gather(group, plan, parts):
    outs = [pltpu.VMEM((len(p) * (QK + VD), parts[0].shape[1]), BF16) for p in plan]
    return pl.pallas_call(
        functools.partial(gather_kernel, group, plan),
        out_shape=outs,
        in_specs=[vmem()] * len(parts),
        out_specs=[vmem()] * len(outs),
        compiler_params=params(8),
        cost_estimate=pl.CostEstimate(flops=1 << 20, transcendentals=0, bytes_accessed=1 << 20),
    )(*parts)


def half_out_kernel(group, *refs):
    pieces, (w_own, out_ref, ctx) = refs[:group], refs[group:]
    own = lax.axis_index("seq") % group
    for d in range(group):
        ctx[:, pl.ds(pl.multiple_of((own ^ d) * VD, VD), VD)] = pieces[d][...]
    out_ref[...] = jnp.dot(ctx[...], w_own[...], preferred_element_type=F32)


def half_out(pieces, w_own):
    group = len(pieces)
    rows, width = pieces[0].shape[0], w_own.shape[1]
    return pl.pallas_call(
        functools.partial(half_out_kernel, group),
        out_shape=pltpu.VMEM((rows, width), F32),
        in_specs=[vmem()] * (group + 1),
        out_specs=vmem(),
        scratch_shapes=[pltpu.VMEM((rows, group * VD), BF16)],
        compiler_params=params(16),
        cost_estimate=pl.CostEstimate(
            flops=2 * rows * width * group * VD, transcendentals=0, bytes_accessed=1 << 20
        ),
        name="half_out",
    )(*pieces, w_own)


def own_tokens_kernel(group, *refs):
    pieces, out_ref = refs[:group], refs[group]
    half = pieces[0].shape[0] // 2
    rows = pl.ds(pl.multiple_of((1 - lax.axis_index("exp")) * half, 16), half)
    for d in range(group):
        out_ref[d * half : (d + 1) * half, :] = pieces[d][rows, :]


def own_tokens(pieces):
    group = len(pieces)
    return pl.pallas_call(
        functools.partial(own_tokens_kernel, group),
        out_shape=pltpu.VMEM((group * pieces[0].shape[0] // 2, pieces[0].shape[1]), BF16),
        in_specs=[vmem()] * group,
        out_specs=vmem(),
        compiler_params=params(8),
        cost_estimate=pl.CostEstimate(flops=1 << 20, transcendentals=0, bytes_accessed=1 << 20),
        name="own_tokens",
    )(*pieces)


def capacity_of(rows):
    return 3 * rows // 4


def slots_of(member, capacity):
    tokens = member.shape[1]
    before = lax.broadcasted_iota(jnp.int32, (tokens, tokens), 0) <= lax.broadcasted_iota(
        jnp.int32, (tokens, tokens), 1
    )
    counted = jnp.dot(
        jnp.broadcast_to(member, (16, tokens)).astype(BF16), before.astype(F32).astype(BF16), preferred_element_type=F32
    )[:1]
    slot = lax.broadcasted_iota(jnp.int32, (capacity, tokens), 0).astype(F32) + F32(1.0)
    return jnp.where((slot == counted) & (member > F32(0.5)), F32(1.0), F32(0.0))


def pack_columns(ref, value):
    rows, width = value.shape
    full = width // 128
    for c in range(full):
        ref[c * rows : (c + 1) * rows, :] = value[:, c * 128 : (c + 1) * 128].astype(BF16)
    rest = value[:, full * 128 :]
    half = rows // 2
    ref[full * rows :, :] = jnp.concatenate([rest[:half], rest[half:]], axis=1).astype(BF16)


def unpack_columns(ref, rows, width):
    full = width // 128
    rest = ref[full * rows :, :].astype(F32)
    rest = jnp.concatenate([rest[:, :64], rest[:, 64:]], axis=0).astype(BF16)
    return jnp.concatenate([ref[c * rows : (c + 1) * rows, :] for c in range(full)] + [rest], axis=1)


def hidden_kernel(group, mine, eps, *refs):
    count = 1 if mine else group
    partial_out, pieces, refs = refs[0], refs[1 : 1 + count], refs[1 + count :]
    w_same, w_swap, gain, gate_w, up_w = refs[:5]
    refs = refs[5:]
    if mine:
        ids, down_own, attended_ref, partial_ref, place_ref, ctx, att = refs
    else:
        hidden_ref, ctx, att = refs
    seq, part = lax.axis_index("seq"), lax.axis_index("exp")
    own = seq % group
    side = seq % 2
    rows_here = ctx.shape[0]
    which = part if mine else 1 - part
    rows = pl.ds(pl.multiple_of(which * rows_here, 16), rows_here)
    half = group * VD
    for d in range(group):
        piece = pieces[0][d * rows_here : (d + 1) * rows_here, :] if mine else pieces[d][...]
        ctx[:, pl.ds(pl.multiple_of((own ^ d) * VD, VD), VD)] = piece
    width = att.shape[1] // 2
    for at, ref in ((side, w_same), (1 - side, w_swap)):
        cols = pl.ds(pl.multiple_of(at * width, 128), width)
        att[:, cols] = partial_out[rows, cols] + jnp.dot(ctx[...], ref[:half, :], preferred_element_type=F32)
    attended = att[...]
    rescale = lax.rsqrt(jnp.mean(attended * attended, axis=1, keepdims=True) + F32(eps))
    normed = (attended * rescale * gain[...]).astype(BF16)
    across = (((1,), (1,)), ((), ()))
    gate = lax.dot_general(gate_w[0], normed, across, preferred_element_type=F32)
    up = lax.dot_general(up_w[0], normed, across, preferred_element_type=F32)
    hidden = (gate * jax.nn.sigmoid(gate) * up).astype(BF16)
    if mine:
        attended_ref[...] = attended
        routed = jnp.where(ids[...] == part, hidden.astype(F32), jnp.zeros(hidden.shape, F32)).astype(BF16)
        partial_ref[...] = jnp.dot(routed.T, down_own[0], preferred_element_type=F32)
        away = jnp.where(ids[...] == part, F32(0.0), F32(1.0))
        place_ref[...] = slots_of(away, place_ref.shape[1]).T.astype(BF16)
    else:
        arriving = w_same[half : half + 1, :rows_here].astype(F32)
        member = jnp.where(arriving == part.astype(F32), F32(1.0), F32(0.0))
        place = slots_of(member, capacity_of(rows_here)).astype(BF16)
        chosen = lax.dot_general(place, hidden, across, preferred_element_type=F32)
        pack_columns(hidden_ref, chosen)


def hidden_part(group, partial_out, pieces, w_same, w_swap, gain, gate_w, up_w, *extra):
    mine = bool(extra)
    rows = partial_out.shape[0] // 2
    width = partial_out.shape[1]
    inner = gate_w.shape[1]
    inputs = [partial_out] + list(pieces) + [w_same, w_swap, gain, gate_w, up_w] + list(extra)
    if mine:
        outs = [pltpu.VMEM((rows, width), F32)] * 2 + [pltpu.VMEM((rows, capacity_of(rows)), BF16)]
    else:
        outs = [pltpu.VMEM((inner * capacity_of(rows) // 128, 128), BF16)]
    return pl.pallas_call(
        functools.partial(hidden_kernel, group, mine, 1e-06),
        out_shape=outs,
        in_specs=[vmem()] * len(inputs),
        out_specs=[vmem()] * len(outs),
        scratch_shapes=[pltpu.VMEM((rows, group * VD), BF16), pltpu.VMEM((rows, width), F32)],
        compiler_params=params(24),
        cost_estimate=pl.CostEstimate(
            flops=2 * rows * width * (2 * group * VD + 2 * inner), transcendentals=rows * inner, bytes_accessed=1 << 20
        ),
        name="hidden_own" if mine else "hidden_peer",
    )(*inputs)


def combine_kernel(group, attended, partial, place, hid_peer, weight, *refs):
    down, out_ref, (result_ref, sem) = refs[:group], refs[group], refs[group + 1 :]
    own = lax.axis_index("seq") % group
    hidden = unpack_columns(hid_peer, place.shape[1], down[0].shape[0])
    other = jnp.dot(place[...], hidden, preferred_element_type=F32).astype(BF16)
    column = jnp.broadcast_to(weight[...], (128, weight.shape[1])).T[:, :1]
    width = out_ref.shape[1] // group
    copies = []
    for d in range(group):
        cols = pl.ds(pl.multiple_of((own ^ d) * width, 128), width)
        result = partial[:, cols] + jnp.dot(other, down[d][...], preferred_element_type=F32)
        result = result.astype(BF16).astype(F32)
        here = slice(d * width, (d + 1) * width)
        result_ref[:, here] = (attended[:, cols] + column * result).astype(BF16)
        copies.append(pltpu.make_async_copy(result_ref.at[:, here], out_ref.at[:, cols], sem.at[d]))
        copies[-1].start()
    for copy in copies:
        copy.wait()


def combine(group, attended, partial, place, hid_peer, weight, down):
    inputs = [attended, partial, place, hid_peer, weight] + list(down)
    return pl.pallas_call(
        functools.partial(combine_kernel, group),
        out_shape=jax.ShapeDtypeStruct(attended.shape, BF16),
        in_specs=[vmem()] * len(inputs),
        out_specs=anywhere(),
        scratch_shapes=[pltpu.VMEM(attended.shape, BF16), pltpu.SemaphoreType.DMA((group,))],
        compiler_params=params(20),
        cost_estimate=pl.CostEstimate(flops=1 << 20, transcendentals=0, bytes_accessed=1 << 20),
        name="combine",
    )(*inputs)


def after(values, *earlier):
    return lax.optimization_barrier((tuple(values), earlier))[0]


def shards(
    queries,
    key_heads,
    value_heads,
    block_layout,
    out_weight,
    norm_gain,
    expert_ids,
    route_weight,
    gate_weight,
    up_weight,
    down_weight,
):
    peers = lax.axis_size("seq")
    group = value_heads.shape[1] // VD
    blocks = queries.shape[0] // BLK
    plane_blocks = group * blocks
    phases = 1 + -(-(SPAN - 1) // plane_blocks)

    def swap(array, d):
        return lax.ppermute(array, "seq", [(i, i ^ d) for i in range(peers)])

    def across(array):
        return lax.ppermute(array, "exp", [(0, 1), (1, 0)])

    def swap_across(array, d):
        pairs = [(2 * i + e, 2 * (i ^ d) + 1 - e) for i in range(peers) for e in range(2)]
        return lax.ppermute(array, ("seq", "exp"), pairs)

    def forward(array):
        return lax.ppermute(array, "seq", [(i, (i + group) % peers) for i in range(peers)])

    def needed(hop):
        return [
            shard
            for shard in range(group)
            if (shard + 1) * blocks - 1 >= plane_blocks * hop - (SPAN - 1)
        ]

    ids = expert_ids.reshape(1, -1)
    kv = pack_kv(key_heads, value_heads, group)
    w_part, down_part = cut(out_weight, down_weight, ids, kv[0], group)
    held = [kv[0]] + [swap(kv[d], d) for d in range(1, group)]
    qs = pack_q(queries, block_layout, kv[0], group, phases)
    qs = [qs[0]] + [swap(qs[d], d) for d in range(1, group)]
    down0 = across(down_part)
    w_same = across(w_part)

    tables = tuple((1, (tuple(g ^ d for g in range(group)),)) for d in range(group))
    early = group // 2
    gate_now, up_now, out_now, down_now = stage(
        (gate_weight.swapaxes(1, 2), up_weight.swapaxes(1, 2), out_weight, down_weight), held[-1]
    )
    q_aug, peak, acc = attend(group, tables, 0, held, q_in=qs)
    down2 = swap(down0, 2)

    parts = held
    for hop in range(1, phases):
        if hop > 1:
            wanted = needed(hop)
            flat = [(at, c, table[c]) for at, (count, table) in enumerate(tables) for c in range(count)]
            chains = []
            for g in range(group):
                there = sorted((f for f in flat if f[2][g] in wanted), key=lambda f: -f[2][g])
                head = [f for f in there if f[0] < early][:1]
                chains.append(head + [f for f in there if f not in head])
            plans = [
                ((tuple((chains[g][k][0], chains[g][k][1]) for g in range(group)),),) for k in range(len(wanted))
            ]
            tables = tuple(
                (1, (tuple(chains[g][k][2][g] for g in range(group)),)) for k in range(len(wanted))
            )
            parts = [gather(group, plan, parts[:early] if k == 0 else parts)[0] for k, plan in enumerate(plans)]
        parts = [forward(part) for part in parts]

        def seen(those):
            highest = max(max(table[c]) for count, table in those for c in range(count))
            limit = highest * blocks + blocks - 1 + SPAN - 1 - plane_blocks * hop
            return tuple(shard for shard in range(group) if shard * blocks <= limit)

        state = (q_aug, peak, acc)
        if hop < phases - 1:
            peak, acc = attend(group, tables, hop, parts, state=state, shards_seen=seen(tables))
        else:
            late = seen(tables[-1:])
            peak, acc, ready = attend(
                group,
                tables[:-1],
                hop,
                parts[:-1],
                state=state,
                shards_seen=seen(tables[:-1]),
                finish=tuple(shard for shard in range(group) if shard not in late),
            )
            context = attend(
                group,
                tables[-1:],
                hop,
                parts[-1:],
                state=(q_aug, peak, acc, ready),
                last=True,
                shards_seen=late,
                finish=late,
            )
    (w_same,) = after((w_same,), context[0])
    w_swap = swap(w_same, 1)
    whole, first = context[:group], context[group : 2 * group]
    same = [whole[0]] + [swap(whole[d], d) for d in range(1, group)]
    other = [across(first[0])] + [swap_across(first[d], d) for d in range(1, group)]
    mine = [across(own_tokens(same))]
    gain = norm_gain.reshape(1, -1)
    partial_out = half_out(same, out_now)
    weights = (w_same, w_swap, gain, gate_now, up_now)
    (hid_out,) = hidden_part(group, partial_out, other, *weights)
    hid_peer = across(hid_out)
    down0, down2 = after((down0, down2), hid_out)
    down1 = swap(down0, 1)
    down3 = swap(down2, 1)
    attended, partial, place = hidden_part(group, partial_out, mine, *weights, ids, down_now)
    return combine(
        group, attended, partial, place, hid_peer, route_weight.reshape(1, -1), (down0, down1, down2, down3)
    )


def solution(mesh):
    in_specs = (
        P("seq", "exp"),
        P("seq", "exp"),
        P("seq", "exp"),
        P("seq", None),
        P("exp", None),
        P(),
        P(("seq", "exp"), None),
        P(("seq", "exp"), None),
        P("exp", None, None),
        P("exp", None, None),
        P("exp", None, None),
    )
    out_specs = P(("seq", "exp"), None)

    return jax.shard_map(shards, mesh=mesh, in_specs=in_specs, out_specs=out_specs, check_vma=False)
```

```python
import functools

import jax
import jax.numpy as jnp
from jax import lax
from jax.experimental import pallas as pl
from jax.experimental.pallas import tpu as pltpu
from jax.sharding import PartitionSpec as P


QK = 192
VD = 128
BLK = 128
SPAN = 22
NEG = -1e30
LOG2E = 1.4426950408889634
F32 = jnp.float32
BF16 = jnp.bfloat16
MIB = 1 << 20
EXTRA = 16


def ceil_to(value, step):
    return -(-value // step) * step


def vmem():
    return pl.BlockSpec(memory_space=pltpu.VMEM)


def params(mib):
    return pltpu.CompilerParams(vmem_limit_bytes=mib * MIB)


def anywhere():
    return pl.BlockSpec(memory_space=pl.ANY)


def in_hbm(array):
    return pltpu.with_memory_space_constraint(array, pltpu.HBM)


def pack_kv_kernel(group, k_ref, v_ref, *refs):
    outs, (k_buf, kt, sem) = refs[:group], refs[group:]
    own = lax.axis_index("seq") % group
    tokens = k_ref.shape[0]
    blocks = tokens // BLK
    loads = []
    for t in range(blocks):
        rows = slice(t * BLK, (t + 1) * BLK)
        loads.append(pltpu.make_async_copy(k_ref.at[rows, :], k_buf.at[rows, :], sem.at[t]))
    stores = []
    for d in range(group):
        cols = pl.ds(pl.multiple_of((own ^ d) * VD, VD), VD)
        for t in range(blocks):
            rows = slice(t * BLK, (t + 1) * BLK)
            stores.append(
                pltpu.make_async_copy(
                    v_ref.at[rows, cols], outs[d].at[QK : QK + VD, rows], sem.at[blocks * (d + 1) + t]
                )
            )
    for copy in loads + stores:
        copy.start()
    for t in range(blocks):
        rows = slice(t * BLK, (t + 1) * BLK)
        loads[t].wait()
        kt[:, rows] = k_buf[rows, :].T
    for d in range(group):
        outs[d][:QK, :] = kt[pl.ds(pl.multiple_of((own ^ d) * QK, 16), QK), :]
    for copy in stores:
        copy.wait()


def pack_kv(k, v, group):
    tokens = k.shape[0]
    return pl.pallas_call(
        functools.partial(pack_kv_kernel, group),
        out_shape=[pltpu.VMEM((QK + VD, tokens), BF16)] * group,
        in_specs=[anywhere()] * 2,
        out_specs=[vmem()] * group,
        scratch_shapes=[
            pltpu.VMEM(k.shape, BF16),
            pltpu.VMEM((k.shape[1], tokens), BF16),
            pltpu.SemaphoreType.DMA(((group + 1) * (tokens // BLK),)),
        ],
        compiler_params=params(8),
        cost_estimate=pl.CostEstimate(flops=1 << 20, transcendentals=0, bytes_accessed=1 << 20),
        name="pack_kv",
    )(in_hbm(k), in_hbm(v))


def cut_kernel(group, w_ref, down_ref, ids_ref, after_ref, w1_out, w2_out, down_out, ids_buf, sem):
    seq = lax.axis_index("seq")
    own = seq % group
    rows, width = w_ref.shape[0], w1_out.shape[1]
    quarter = down_out.shape[1]
    first = (seq % 2) * (8 * width)
    outer = first + (seq // 2 % 2) * (7 * width)
    ids_load = pltpu.make_async_copy(ids_ref, ids_buf, sem.at[0])
    copies = [
        pltpu.make_async_copy(
            w_ref.at[:, pl.ds(pl.multiple_of(outer, 128), width)], w1_out.at[:rows, :], sem.at[1]
        ),
        pltpu.make_async_copy(
            down_ref.at[0, :, pl.ds(pl.multiple_of(own * quarter, 128), quarter)], down_out, sem.at[2]
        ),
        pltpu.make_async_copy(
            w_ref.at[:, pl.ds(pl.multiple_of(first + width, 128), 6 * width)], w2_out, sem.at[3]
        ),
    ]
    for copy in [ids_load] + copies:
        copy.start()
    ids_load.wait()
    ids = jnp.broadcast_to(ids_buf[...].astype(F32), (EXTRA, ids_buf.shape[1]))
    columns = jnp.concatenate([ids, jnp.zeros((EXTRA, 2 * width - ids.shape[1]), F32)], axis=1)
    w1_out[rows : rows + EXTRA, :] = columns[:, :width].astype(BF16)
    w1_out[rows + EXTRA :, :] = columns[:, width:].astype(BF16)
    for copy in copies:
        copy.wait()


def cut(w, down, ids, earlier, group):
    width = w.shape[1] // 16
    return pl.pallas_call(
        functools.partial(cut_kernel, group),
        out_shape=[
            pltpu.VMEM((w.shape[0] + 2 * EXTRA, width), BF16),
            pltpu.VMEM((w.shape[0], 6 * width), BF16),
            pltpu.VMEM((down.shape[1], down.shape[2] // group), BF16),
        ],
        in_specs=[anywhere()] * 4,
        out_specs=[vmem()] * 3,
        scratch_shapes=[pltpu.VMEM(ids.shape, jnp.int32), pltpu.SemaphoreType.DMA((4,))],
        compiler_params=params(8),
        cost_estimate=pl.CostEstimate(flops=1 << 20, transcendentals=0, bytes_accessed=1 << 20),
        name="cut",
    )(in_hbm(w), in_hbm(down), in_hbm(ids), earlier)


def join_outer_kernel(own_ref, other_ref, out_ref):
    width = own_ref.shape[1]
    far = lax.axis_index("seq") // 2 % 2
    rows = out_ref.shape[0]
    out_ref[:, pl.ds(pl.multiple_of(far * width, 128), width)] = own_ref[:rows, :]
    out_ref[:, pl.ds(pl.multiple_of((1 - far) * width, 128), width)] = other_ref[:rows, :]


def join_outer(own, other):
    return pl.pallas_call(
        join_outer_kernel,
        out_shape=pltpu.VMEM((own.shape[0] - 2 * EXTRA, 2 * own.shape[1]), BF16),
        in_specs=[vmem()] * 2,
        out_specs=vmem(),
        compiler_params=params(8),
        cost_estimate=pl.CostEstimate(flops=1 << 20, transcendentals=0, bytes_accessed=1 << 20),
        name="join_outer",
    )(own, other)


def stage_kernel(*refs):
    count = (len(refs) - 2) // 2
    sem = refs[-1]
    copies = [
        pltpu.make_async_copy(refs[at], refs[count + 1 + at], sem.at[at]) for at in range(count)
    ]
    for copy in copies:
        copy.start()
    for copy in copies:
        copy.wait()


def stage(arrays, earlier):
    return pl.pallas_call(
        stage_kernel,
        out_shape=[pltpu.VMEM(a.shape, a.dtype) for a in arrays],
        in_specs=[anywhere()] * (len(arrays) + 1),
        out_specs=[vmem()] * len(arrays),
        scratch_shapes=[pltpu.SemaphoreType.DMA((len(arrays),))],
        compiler_params=params(16),
        cost_estimate=pl.CostEstimate(flops=1 << 20, transcendentals=0, bytes_accessed=1 << 20),
        name="stage",
    )(*[in_hbm(a) for a in arrays], earlier)


def pack_q_kernel(group, phases, layout_hbm, q_ref, after_ref, *refs):
    outs, (layout_ref, q_buf, qt, sem) = refs[:group], refs[group:]
    seq = lax.axis_index("seq")
    own, plane = seq % group, seq // group
    tokens = q_ref.shape[0]
    blocks, chosen = layout_ref.shape
    plane_blocks = group * blocks
    aug = outs[0].shape[0] - QK
    loads = []
    for t in range(tokens // BLK):
        rows = slice(t * BLK, (t + 1) * BLK)
        loads.append(pltpu.make_async_copy(q_ref.at[rows, :], q_buf.at[rows, :], sem.at[t]))
    layout_load = pltpu.make_async_copy(layout_hbm, layout_ref, sem.at[blocks])
    for copy in [layout_load] + loads:
        copy.start()
    row = lax.broadcasted_iota(jnp.int32, (aug, BLK), 0)
    phase = jnp.zeros_like(row)
    for p in range(1, phases):
        phase = phase + (row >= p * plane_blocks).astype(jnp.int32)
    exists = (phase <= plane) & (row < phases * plane_blocks)
    layout_load.wait()
    for t in range(tokens // BLK):
        rows = slice(t * BLK, (t + 1) * BLK)
        offset = own * blocks + t + 2 * plane_blocks * phase - row
        hit = offset == layout_ref[t, 0]
        for c in range(1, chosen):
            hit = hit | (offset == layout_ref[t, c])
        mask = jnp.where(hit & exists, F32(0.0), F32(NEG)).astype(BF16)
        for d in range(group):
            outs[d][QK:, rows] = mask
        loads[t].wait()
        qt[:, rows] = q_buf[rows, :].T
    for d in range(group):
        outs[d][:QK, :] = qt[pl.ds(pl.multiple_of((own ^ d) * QK, 16), QK), :]


def pack_q(q, layout, earlier, group, phases):
    tokens = q.shape[0]
    aug = ceil_to(phases * group * layout.shape[0], 16)
    return pl.pallas_call(
        functools.partial(pack_q_kernel, group, phases),
        out_shape=[pltpu.VMEM((QK + aug, tokens), BF16)] * group,
        in_specs=[anywhere()] * 3,
        out_specs=[vmem()] * group,
        scratch_shapes=[
            pltpu.SMEM(layout.shape, jnp.int32),
            pltpu.VMEM(q.shape, BF16),
            pltpu.VMEM((q.shape[1], tokens), BF16),
            pltpu.SemaphoreType.DMA((layout.shape[0] + 1,)),
        ],
        compiler_params=params(8),
        cost_estimate=pl.CostEstimate(flops=1 << 20, transcendentals=0, bytes_accessed=1 << 20),
        name="pack_q",
    )(in_hbm(layout), in_hbm(q), earlier)


def select_index(values, own):
    picked = jnp.int32(values[0])
    for at in range(1, len(values)):
        picked = jnp.where(own == at, jnp.int32(values[at]), picked)
    return picked


def attend_kernel(group, tables, phase, first, last, shards_seen, finish, rows_step, *refs):
    refs = list(refs)

    def take(count):
        taken = refs[:count]
        del refs[:count]
        return taken

    if first:
        q_in = take(group)
    else:
        q_ref, m_in, acc_in = take(3)
        if last:
            (ready,) = take(1)
    kv_refs = take(len(tables))
    if first:
        q_ref, m_out, acc_out = take(3)
    elif last:
        outs = take(2 * group)
        (context,) = take(1)
    else:
        m_out, acc_out = take(2)
        if finish:
            (context,) = take(1)
    kaug, vaug, s_ref = refs
    own = lax.axis_index("seq") % group
    tokens = kv_refs[0].shape[1]
    blocks = tokens // BLK
    aug = kaug.shape[0] - QK
    scale = F32(QK**-0.5 * LOG2E)
    if first:
        depth = q_in[0].shape[0]
        for d in range(group):
            for t in range(blocks):
                rows = slice(d * tokens + t * BLK, d * tokens + (t + 1) * BLK)
                q_ref[rows, :depth] = q_in[d][:, t * BLK : (t + 1) * BLK].T
                if depth < q_ref.shape[1]:
                    q_ref[rows, depth:] = jnp.zeros((BLK, q_ref.shape[1] - depth), BF16)
    row = lax.broadcasted_iota(jnp.int32, (aug, BLK), 0)
    at = 0
    for (count, table), ref in zip(tables, kv_refs):
        for c in range(count):
            base = c * (QK + VD)
            kaug[:QK, at * tokens : (at + 1) * tokens] = ref[base : base + QK, :]
            shard = select_index(table[c], own)
            for t in range(blocks):
                part = slice(at * tokens + t * BLK, at * tokens + (t + 1) * BLK)
                here = (phase * group + shard) * blocks + t
                kaug[QK:, part] = jnp.where(row == here, F32(1.0), F32(0.0)).astype(BF16)
                vaug[part, :VD] = ref[base + QK : base + QK + VD, t * BLK : (t + 1) * BLK]
                vaug[part, VD:] = jnp.ones((BLK, VD), BF16)
            at += 1

    def step(rows, slot, diagonal, done):
        s_now = s_ref.at[slot]
        s_now[...] = jnp.dot(q_ref[rows, :], kaug[...], preferred_element_type=F32)
        if first:
            lower = lax.broadcasted_iota(jnp.int32, (BLK, BLK), 0) >= lax.broadcasted_iota(
                jnp.int32, (BLK, BLK), 1
            )
            for t in range(rows_step // BLK):
                tile = (slice(t * BLK, (t + 1) * BLK), slice(diagonal + t * BLK, diagonal + (t + 1) * BLK))
                s_now[tile] = jnp.where(lower, s_now[tile], F32(NEG))
        peak = jnp.max(s_now[...], axis=1, keepdims=True)
        if not first:
            before = m_in[rows, :1]
            peak = jnp.maximum(peak, before)
        weights = jnp.exp2((s_now[...] - peak) * scale).astype(BF16)
        acc = jnp.dot(weights, vaug[...], preferred_element_type=F32)
        if not first:
            acc = acc + acc_in[rows, :] * jnp.exp2((before - peak) * scale)
        if done:
            context[rows, :] = (acc[:, :VD] / acc[:, VD:]).astype(BF16)
        else:
            m_out[rows, :] = jnp.broadcast_to(peak, (rows_step, m_out.shape[1]))
            acc_out[rows, :] = acc

    per = tokens // rows_step
    count = 0
    for shard in range(group):
        for r in range(per):
            if first:
                start = shard * tokens + r * rows_step
                step(slice(start, start + rows_step), count % 2, start, False)
                count += 1
                continue
            rows = pl.ds(pl.multiple_of((own ^ shard) * tokens + r * rows_step, rows_step), rows_step)
            if shard in shards_seen:
                step(rows, count % 2, 0, shard in finish)
                count += 1
            elif shard in finish:
                context[rows, :] = (acc_in[rows, :VD] / acc_in[rows, VD:]).astype(BF16)
    if last:
        half = tokens // 2
        part = lax.axis_index("exp")
        for d in range(group):
            outs[d][...] = context[d * tokens : (d + 1) * tokens, :]
            at = pl.multiple_of(d * tokens + part * half, 16)
            outs[group + d][...] = context[pl.ds(at, half), :]


def attend(group, tables, phase, kv, q_in=None, state=None, last=False, shards_seen=(), finish=(), rows_step=128):
    first = state is None
    tokens = kv[0].shape[1]
    total = group * tokens
    keys = sum(count for count, _ in tables) * tokens
    depth = q_in[0].shape[0] if first else state[0].shape[1]
    depth = ceil_to(depth, 128)
    outs = [pltpu.VMEM((total, 128), F32), pltpu.VMEM((total, 2 * VD), F32)]
    scratch = [
        pltpu.VMEM((depth, keys), BF16),
        pltpu.VMEM((keys, 2 * VD), BF16),
        pltpu.VMEM((2, rows_step, keys), F32),
    ]
    aliases = {}
    if first:
        inputs = list(q_in)
        outs = [pltpu.VMEM((total, depth), BF16)] + outs
    elif last:
        inputs = list(state)
        outs = [pltpu.VMEM((tokens, VD), BF16)] * group + [pltpu.VMEM((tokens // 2, VD), BF16)] * group
        outs = outs + [pltpu.VMEM((total, VD), BF16)]
        aliases = {3: 2 * group}
    else:
        inputs = list(state)
        aliases = {1: 0, 2: 1}
        if finish:
            outs = outs + [pltpu.VMEM((total, VD), BF16)]
    inputs = inputs + list(kv)
    queries = total if first else len(shards_seen) * tokens
    return pl.pallas_call(
        functools.partial(attend_kernel, group, tables, phase, first, last, shards_seen, finish, rows_step),
        out_shape=outs,
        in_specs=[vmem()] * len(inputs),
        out_specs=[vmem()] * len(outs),
        scratch_shapes=scratch,
        input_output_aliases=aliases,
        compiler_params=params(20),
        cost_estimate=pl.CostEstimate(
            flops=4 * queries * keys * 256, transcendentals=queries * keys, bytes_accessed=1 << 20
        ),
    )(*inputs)


def gather_kernel(group, plan, *refs):
    parts, outs = refs[: -len(plan)], refs[-len(plan) :]
    own = lax.axis_index("seq") % group
    size = QK + VD
    for g in range(group):

        @pl.when(own == g)
        def _():
            for out, places in zip(outs, plan):
                for at, place in enumerate(places):
                    part, c = place[g]
                    out[at * size : (at + 1) * size, :] = parts[part][c * size : (c + 1) * size, :]


def gather(group, plan, parts):
    outs = [pltpu.VMEM((len(p) * (QK + VD), parts[0].shape[1]), BF16) for p in plan]
    return pl.pallas_call(
        functools.partial(gather_kernel, group, plan),
        out_shape=outs,
        in_specs=[vmem()] * len(parts),
        out_specs=[vmem()] * len(outs),
        compiler_params=params(8),
        cost_estimate=pl.CostEstimate(flops=1 << 20, transcendentals=0, bytes_accessed=1 << 20),
    )(*parts)


def half_out_kernel(group, *refs):
    pieces, (w_own, out_ref, ctx) = refs[:group], refs[group:]
    own = lax.axis_index("seq") % group
    for d in range(group):
        ctx[:, pl.ds(pl.multiple_of((own ^ d) * VD, VD), VD)] = pieces[d][...]
    out_ref[...] = jnp.dot(ctx[...], w_own[...], preferred_element_type=F32)


def half_out(pieces, w_own):
    group = len(pieces)
    rows, width = pieces[0].shape[0], w_own.shape[1]
    return pl.pallas_call(
        functools.partial(half_out_kernel, group),
        out_shape=pltpu.VMEM((rows, width), F32),
        in_specs=[vmem()] * (group + 1),
        out_specs=vmem(),
        scratch_shapes=[pltpu.VMEM((rows, group * VD), BF16)],
        compiler_params=params(16),
        cost_estimate=pl.CostEstimate(
            flops=2 * rows * width * group * VD, transcendentals=0, bytes_accessed=1 << 20
        ),
        name="half_out",
    )(*pieces, w_own)


def own_tokens_kernel(group, *refs):
    pieces, out_ref = refs[:group], refs[group]
    half = pieces[0].shape[0] // 2
    rows = pl.ds(pl.multiple_of((1 - lax.axis_index("exp")) * half, 16), half)
    for d in range(group):
        out_ref[d * half : (d + 1) * half, :] = pieces[d][rows, :]


def own_tokens(pieces):
    group = len(pieces)
    return pl.pallas_call(
        functools.partial(own_tokens_kernel, group),
        out_shape=pltpu.VMEM((group * pieces[0].shape[0] // 2, pieces[0].shape[1]), BF16),
        in_specs=[vmem()] * group,
        out_specs=vmem(),
        compiler_params=params(8),
        cost_estimate=pl.CostEstimate(flops=1 << 20, transcendentals=0, bytes_accessed=1 << 20),
        name="own_tokens",
    )(*pieces)


def capacity_of(rows):
    return 3 * rows // 4


def slots_of(member, capacity):
    tokens = member.shape[1]
    before = lax.broadcasted_iota(jnp.int32, (tokens, tokens), 0) <= lax.broadcasted_iota(
        jnp.int32, (tokens, tokens), 1
    )
    counted = jnp.dot(
        jnp.broadcast_to(member, (16, tokens)).astype(BF16), before.astype(F32).astype(BF16), preferred_element_type=F32
    )[:1]
    slot = lax.broadcasted_iota(jnp.int32, (capacity, tokens), 0).astype(F32) + F32(1.0)
    return jnp.where((slot == counted) & (member > F32(0.5)), F32(1.0), F32(0.0))


def pack_columns(ref, value):
    rows, width = value.shape
    full = width // 128
    for c in range(full):
        ref[c * rows : (c + 1) * rows, :] = value[:, c * 128 : (c + 1) * 128].astype(BF16)
    rest = value[:, full * 128 :]
    half = rows // 2
    ref[full * rows :, :] = jnp.concatenate([rest[:half], rest[half:]], axis=1).astype(BF16)


def unpack_columns(ref, rows, width):
    full = width // 128
    rest = ref[full * rows :, :].astype(F32)
    rest = jnp.concatenate([rest[:, :64], rest[:, 64:]], axis=0).astype(BF16)
    return jnp.concatenate([ref[c * rows : (c + 1) * rows, :] for c in range(full)] + [rest], axis=1)


def hidden_kernel(group, mine, eps, *refs):
    count = 1 if mine else group
    partial_out, pieces, refs = refs[0], refs[1 : 1 + count], refs[1 + count :]
    outer, outer_core, inner, inner_core, ids_row, gain, gate_w, up_w = refs[:8]
    refs = refs[8:]
    if mine:
        ids, down_own, attended_ref, partial_ref, place_ref, ctx, att = refs
    else:
        hidden_ref, ctx, att = refs
    seq, part = lax.axis_index("seq"), lax.axis_index("exp")
    own = seq % group
    side = seq % 2
    rows_here = ctx.shape[0]
    which = part if mine else 1 - part
    rows = pl.ds(pl.multiple_of(which * rows_here, 16), rows_here)
    half = group * VD
    for d in range(group):
        piece = pieces[0][d * rows_here : (d + 1) * rows_here, :] if mine else pieces[d][...]
        ctx[:, pl.ds(pl.multiple_of((own ^ d) * VD, VD), VD)] = piece
    width = att.shape[1] // 16
    for at, edges, middle in ((side, outer, inner), (1 - side, outer_core, inner_core)):
        for begin, ref in ((0, edges.at[:, :width]), (1, middle), (7, edges.at[:, width:])):
            cols = pl.ds(pl.multiple_of((8 * at + begin) * width, 128), ref.shape[1])
            att[:, cols] = partial_out[rows, cols] + jnp.dot(ctx[...], ref[...], preferred_element_type=F32)
    attended = att[...]
    rescale = lax.rsqrt(jnp.mean(attended * attended, axis=1, keepdims=True) + F32(eps))
    normed = (attended * rescale * gain[...]).astype(BF16)
    across = (((1,), (1,)), ((), ()))
    gate = lax.dot_general(gate_w[0], normed, across, preferred_element_type=F32)
    up = lax.dot_general(up_w[0], normed, across, preferred_element_type=F32)
    hidden = (gate * jax.nn.sigmoid(gate) * up).astype(BF16)
    if mine:
        attended_ref[...] = attended
        routed = jnp.where(ids[...] == part, hidden.astype(F32), jnp.zeros(hidden.shape, F32)).astype(BF16)
        partial_ref[...] = jnp.dot(routed.T, down_own[0], preferred_element_type=F32)
        away = jnp.where(ids[...] == part, F32(0.0), F32(1.0))
        place_ref[...] = slots_of(away, place_ref.shape[1]).T.astype(BF16)
    else:
        arriving = jnp.concatenate([ids_row[half : half + 1, :], ids_row[half + EXTRA : half + EXTRA + 1, :]], axis=1)
        arriving = arriving[:, :rows_here].astype(F32)
        member = jnp.where(arriving == part.astype(F32), F32(1.0), F32(0.0))
        place = slots_of(member, capacity_of(rows_here)).astype(BF16)
        chosen = lax.dot_general(place, hidden, across, preferred_element_type=F32)
        pack_columns(hidden_ref, chosen)


def hidden_part(group, partial_out, pieces, w_parts, gain, gate_w, up_w, *extra):
    mine = bool(extra)
    rows = partial_out.shape[0] // 2
    width = partial_out.shape[1]
    inner = gate_w.shape[1]
    inputs = [partial_out] + list(pieces) + list(w_parts) + [gain, gate_w, up_w] + list(extra)
    if mine:
        outs = [pltpu.VMEM((rows, width), F32)] * 2 + [pltpu.VMEM((rows, capacity_of(rows)), BF16)]
    else:
        outs = [pltpu.VMEM((inner * capacity_of(rows) // 128, 128), BF16)]
    return pl.pallas_call(
        functools.partial(hidden_kernel, group, mine, 1e-06),
        out_shape=outs,
        in_specs=[vmem()] * len(inputs),
        out_specs=[vmem()] * len(outs),
        scratch_shapes=[pltpu.VMEM((rows, group * VD), BF16), pltpu.VMEM((rows, width), F32)],
        compiler_params=params(24),
        cost_estimate=pl.CostEstimate(
            flops=2 * rows * width * (2 * group * VD + 2 * inner), transcendentals=rows * inner, bytes_accessed=1 << 20
        ),
        name="hidden_own" if mine else "hidden_peer",
    )(*inputs)


def combine_kernel(group, attended, partial, place, hid_peer, weight, *refs):
    down, out_ref, (result_ref, sem) = refs[:group], refs[group], refs[group + 1 :]
    own = lax.axis_index("seq") % group
    hidden = unpack_columns(hid_peer, place.shape[1], down[0].shape[0])
    other = jnp.dot(place[...], hidden, preferred_element_type=F32).astype(BF16)
    column = jnp.broadcast_to(weight[...], (128, weight.shape[1])).T[:, :1]
    width = out_ref.shape[1] // group
    copies = []
    for d in range(group):
        cols = pl.ds(pl.multiple_of((own ^ d) * width, 128), width)
        result = partial[:, cols] + jnp.dot(other, down[d][...], preferred_element_type=F32)
        result = result.astype(BF16).astype(F32)
        here = slice(d * width, (d + 1) * width)
        result_ref[:, here] = (attended[:, cols] + column * result).astype(BF16)
        copies.append(pltpu.make_async_copy(result_ref.at[:, here], out_ref.at[:, cols], sem.at[d]))
        copies[-1].start()
    for copy in copies:
        copy.wait()


def combine(group, attended, partial, place, hid_peer, weight, down):
    inputs = [attended, partial, place, hid_peer, weight] + list(down)
    return pl.pallas_call(
        functools.partial(combine_kernel, group),
        out_shape=jax.ShapeDtypeStruct(attended.shape, BF16),
        in_specs=[vmem()] * len(inputs),
        out_specs=anywhere(),
        scratch_shapes=[pltpu.VMEM(attended.shape, BF16), pltpu.SemaphoreType.DMA((group,))],
        compiler_params=params(20),
        cost_estimate=pl.CostEstimate(flops=1 << 20, transcendentals=0, bytes_accessed=1 << 20),
        name="combine",
    )(*inputs)


def after(values, *earlier):
    return lax.optimization_barrier((tuple(values), earlier))[0]


def shards(
    queries,
    key_heads,
    value_heads,
    block_layout,
    out_weight,
    norm_gain,
    expert_ids,
    route_weight,
    gate_weight,
    up_weight,
    down_weight,
):
    peers = lax.axis_size("seq")
    group = value_heads.shape[1] // VD
    blocks = queries.shape[0] // BLK
    plane_blocks = group * blocks
    phases = 1 + -(-(SPAN - 1) // plane_blocks)

    def swap(array, d):
        return lax.ppermute(array, "seq", [(i, i ^ d) for i in range(peers)])

    def across(array):
        return lax.ppermute(array, "exp", [(0, 1), (1, 0)])

    def swap_across(array, d):
        pairs = [(2 * i + e, 2 * (i ^ d) + 1 - e) for i in range(peers) for e in range(2)]
        return lax.ppermute(array, ("seq", "exp"), pairs)

    def forward(array, final):
        pairs = [(i, (i + group) % peers) for i in range(peers)]
        if final:
            pairs = [(i, i + group) for i in range((phases - 2) * group, peers - group)]
        return lax.ppermute(array, "seq", pairs)

    def needed(hop):
        return [
            shard
            for shard in range(group)
            if (shard + 1) * blocks - 1 >= plane_blocks * hop - (SPAN - 1)
        ]

    ids = expert_ids.reshape(1, -1)
    kv = pack_kv(key_heads, value_heads, group)
    w1_part, w2_part, down_part = cut(out_weight, down_weight, ids, kv[0], group)
    held = [kv[0]] + [swap(kv[d], d) for d in range(1, group)]
    qs = pack_q(queries, block_layout, kv[0], group, phases)
    qs = [qs[0]] + [swap(qs[d], d) for d in range(1, group)]
    down0 = across(down_part)
    w1 = across(w1_part)
    w2 = across(w2_part)
    outer = join_outer(w1, swap(w1, 2))

    tables = tuple((1, (tuple(g ^ d for g in range(group)),)) for d in range(group))
    early = group // 2
    gate_now, up_now, out_now, down_now = stage(
        (gate_weight.swapaxes(1, 2), up_weight.swapaxes(1, 2), out_weight, down_weight), held[-1]
    )
    q_aug, peak, acc = attend(group, tables, 0, held, q_in=qs)
    down2 = swap(down0, 2)

    parts = held
    for hop in range(1, phases):
        if hop > 1:
            wanted = needed(hop)
            flat = [(at, c, table[c]) for at, (count, table) in enumerate(tables) for c in range(count)]
            chains = []
            for g in range(group):
                there = sorted((f for f in flat if f[2][g] in wanted), key=lambda f: -f[2][g])
                head = [f for f in there if f[0] < early][:1]
                chains.append(head + [f for f in there if f not in head])
            plans = [
                ((tuple((chains[g][k][0], chains[g][k][1]) for g in range(group)),),) for k in range(len(wanted))
            ]
            tables = tuple(
                (1, (tuple(chains[g][k][2][g] for g in range(group)),)) for k in range(len(wanted))
            )
            parts = [gather(group, plan, parts[:early] if k == 0 else parts)[0] for k, plan in enumerate(plans)]
        final = len(parts) - 1 if hop == phases - 1 else -1
        parts = [forward(part, at == final) for at, part in enumerate(parts)]

        def seen(those):
            highest = max(max(table[c]) for count, table in those for c in range(count))
            limit = highest * blocks + blocks - 1 + SPAN - 1 - plane_blocks * hop
            return tuple(shard for shard in range(group) if shard * blocks <= limit)

        state = (q_aug, peak, acc)
        if hop < phases - 1:
            peak, acc = attend(group, tables, hop, parts, state=state, shards_seen=seen(tables))
        else:
            late = seen(tables[-1:])
            peak, acc, ready = attend(
                group,
                tables[:-1],
                hop,
                parts[:-1],
                state=state,
                shards_seen=seen(tables[:-1]),
                finish=tuple(shard for shard in range(group) if shard not in late),
            )
            context = attend(
                group,
                tables[-1:],
                hop,
                parts[-1:],
                state=(q_aug, peak, acc, ready),
                last=True,
                shards_seen=late,
                finish=late,
            )
    outer_core = swap(outer, 1)
    whole, first = context[:group], context[group : 2 * group]
    same = [whole[0]] + [swap(whole[d], d) for d in range(1, group)]
    other = [across(first[0])] + [swap_across(first[d], d) for d in range(1, group)]
    (w2,) = after((w2,), same[1])
    w2_core = swap(w2, 1)
    mine = [across(own_tokens(same))]
    gain = norm_gain.reshape(1, -1)
    partial_out = half_out(same, out_now)
    weights = ((outer, outer_core, w2, w2_core, w1), gain, gate_now, up_now)
    (hid_out,) = hidden_part(group, partial_out, other, *weights)
    hid_peer = across(hid_out)
    down0, down2 = after((down0, down2), hid_out)
    down1 = swap(down0, 1)
    down3 = swap(down2, 1)
    attended, partial, place = hidden_part(group, partial_out, mine, *weights, ids, down_now)
    return combine(
        group, attended, partial, place, hid_peer, route_weight.reshape(1, -1), (down0, down1, down2, down3)
    )


def solution(mesh):
    in_specs = (
        P("seq", "exp"),
        P("seq", "exp"),
        P("seq", "exp"),
        P("seq", None),
        P("exp", None),
        P(),
        P(("seq", "exp"), None),
        P(("seq", "exp"), None),
        P("exp", None, None),
        P("exp", None, None),
        P("exp", None, None),
    )
    out_specs = P(("seq", "exp"), None)

    return jax.shard_map(shards, mesh=mesh, in_specs=in_specs, out_specs=out_specs, check_vma=False)
```
